32 devices in a mesh: seq: 16 (over z, y, core), head: 2 (over x).
Axes of the slice: x: 2, y: 2, z: 4, core: 2. Of those that a mesh axis runs over, the one named last changes fastest.
Arguments:
- tokens: bfloat16 [1, 8192, 2048], P(None, 'seq'), may hold values from -6 to 6
- qkv_weight: bfloat16 [2048, 3, 2048], P(None, None, 'head'), may hold values from -1 to 1
- persistent: bfloat16 [2, 128, 2048], P(None, None, 'head'), may hold values from -60 to 60
- rate_weight: float32 [2048], replicated, may hold values from -0.25 to 0.25
- forget_rate: float32 [1, 8192], P(None, 'seq'), may hold values from 9.765625e-07 to 0.0009765625
- momentum_decay: float32 [1], replicated, may hold values from 0.5 to 0.95
- forget_share: float32 [1], replicated, may hold values from 0.05 to 0.5
- memory: float32 [2048, 2, 4096], P('seq', None, 'head'), may hold values from -0.125 to 0.125
- momentum: float32 [2048, 2, 4096], P('seq', None, 'head'), may hold values from -0.0625 to 0.0625
Outputs:
- attended: bfloat16 [1, 8192, 2048], P(None, 'seq', 'head')
- memory_out: float32 [2048, 2, 4096], P('seq', None, 'head')
- momentum_out: float32 [2048, 2, 4096], P('seq', None, 'head')
The draws below stay inside these ranges and needn't reach their ends.
All inputs are finite; a program needn't handle non-finite values.
Results may differ from the reference program's by a relative error of at most 0.01.
Values may be sent and summed in bfloat16 or wider, within the bound.
A program may use at most 128 MiB of HBM per device.

```python
import math
import jax
import jax.numpy as jnp
from jax import lax

D = 2048
HEADS = 16
HEAD_DIM = 128
MEM_UNITS = 4096
NP = 128
TOK_DEV = 512
BLOCKS = 1
TOKENS_STEP = 8192
N_SEQ = 16
N_HEAD = 2


def qkv_draw(key):
    raw_weights = jax.random.normal(jax.random.fold_in(key, 102), (D, 3, D), jnp.float32)
    return jnp.clip(raw_weights, -6.0, 6.0) * D ** (-0.5)


def draw_tokens(key, part):
    token_noise = jax.random.normal(jax.random.fold_in(key, 103), (BLOCKS, TOKENS_STEP, D), jnp.float32)
    values_all = token_noise
    return jnp.clip(values_all, -6.0, 6.0).astype(jnp.bfloat16)


def draw_qkv_weight(key, part):
    return qkv_draw(key).astype(jnp.bfloat16)


def draw_persistent(key, part):
    base_rows = jnp.clip(jax.random.normal(jax.random.fold_in(key, 104), (2, NP, D), jnp.float32), -6.0, 6.0)
    return base_rows.astype(jnp.bfloat16)


def level_of(own_key, shape, split, smallest, high):
    factor_of, own = 1.0, jax.random.fold_in(own_key, 6)
    for dim, blocks in split:
        draws = jnp.exp(jax.random.uniform(jax.random.fold_in(own, dim), (blocks,), jnp.float32, smallest / len(split), high / len(split)))
        factor_of = factor_of * jnp.repeat(draws, shape[dim] // blocks).reshape([-1 if axis == dim else 1 for axis in range(len(shape))])
    return factor_of


def centred(own_key, extent, deviation, reach, shards=(), kind=jnp.bfloat16):
    entries = jax.random.normal(own_key, extent, jnp.float32) * deviation
    if len(shards) > 0:
        entries = level_of(own_key, extent, shards, -0.22, 0.18) * entries
    return jnp.clip(entries, min=-reach, max=reach).astype(kind)


def setup_inputs(seed: int = 0) -> dict:
    key_of = jax.random.split(jax.random.key(seed), 10)
    tokens = draw_tokens(jax.random.fold_in(key_of[9], 71), 0)
    qkv_weight = draw_qkv_weight(jax.random.fold_in(key_of[9], 71), 0)
    persistent = draw_persistent(jax.random.fold_in(key_of[9], 71), 0)
    rate_weight = centred(key_of[3], (D,), (D // 4) ** -0.5, 0.25, (), jnp.float32)
    forget_rate = jnp.clip(jnp.exp(math.log(0.0009765625) - 6.9077552 * jax.random.uniform(key_of[4], (BLOCKS, TOKENS_STEP), jnp.float32) ** level_of(key_of[4], (BLOCKS, TOKENS_STEP), ((1, 16),), -0.2, 0.2)), 9.765625463842298e-07, 0.0009765625)
    momentum_decay = jnp.clip(jax.random.uniform(key_of[5], (BLOCKS,), jnp.float32, 0.5, 0.95), 0.5, 0.95)
    forget_share = jnp.clip(jax.random.uniform(key_of[6], (BLOCKS,), jnp.float32, 0.05, 0.5), 0.05, 0.5)
    memory = centred(key_of[7], (D, 2, MEM_UNITS), D ** -0.5, 0.125, ((0, 16), (2, 2)), jnp.float32)
    momentum = centred(key_of[8], (D, 2, MEM_UNITS), (4 * D) ** -0.5, 0.0625, ((0, 16), (2, 2)), jnp.float32)
    return {"tokens": tokens, "qkv_weight": qkv_weight, "persistent": persistent, "rate_weight": rate_weight, "forget_rate": forget_rate, "momentum_decay": momentum_decay, "forget_share": forget_share, "memory": memory, "momentum": momentum}


def key_mask(count, persist_count):
    rows_at = jnp.arange(count)[:, None]
    column = jnp.arange(persist_count + 2 * count)[None, :]
    local_pos = jnp.where(column < persist_count + count, column - persist_count, column - persist_count - count)
    return (column < persist_count) | (local_pos <= rows_at)


def attend_segment(parts, persist_keys, persist_values):
    query, keys, values, recalled = parts
    count = query.shape[0]
    all_keys = jnp.concatenate([persist_keys, recalled, keys], axis=0)
    all_values = jnp.concatenate([persist_values, recalled, values], axis=0)
    scores = jnp.einsum("thd,nhd->htn", query.astype(jnp.float32), all_keys.astype(jnp.float32)) * (HEAD_DIM ** -0.5)
    visible = key_mask(count, persist_keys.shape[0])
    scores = jnp.where(visible[None], scores, -1e30)
    largest = jnp.max(scores, axis=2, keepdims=True)
    expo = jnp.exp(scores - largest)
    probs = (expo / jnp.sum(expo, axis=2, keepdims=True)).astype(jnp.bfloat16)
    result = jnp.einsum("htn,nhd->thd", probs.astype(jnp.float32), all_values.astype(jnp.float32))
    return result.astype(jnp.bfloat16)


def reference(tokens, qkv_weight, persistent, rate_weight, forget_rate, momentum_decay, forget_share, memory, momentum):
    steps_len = TOKENS_STEP
    group = MEM_UNITS // N_HEAD
    lr_scale = 2.0 / (D * steps_len) ** 0.5
    tail = jnp.sum(forget_rate, axis=1, keepdims=True) - jnp.cumsum(forget_rate, axis=1)
    persist_keys = persistent[0].reshape(NP, HEADS, HEAD_DIM)
    persist_values = persistent[1].reshape(NP, HEADS, HEAD_DIM)
    results = []
    for block in range(BLOCKS):
        inputs = tokens[block]
        proj = jnp.einsum("td,dkf->tkf", inputs.astype(jnp.float32), qkv_weight.astype(jnp.float32)).astype(jnp.bfloat16)
        query, keys, values = proj[:, 0], proj[:, 1], proj[:, 2]
        weights_low = memory.astype(jnp.bfloat16)
        first, second = weights_low[:, 0, :], weights_low[:, 1, :]
        stacked = jnp.concatenate([query, keys], axis=0)
        preact = jnp.dot(stacked, first, preferred_element_type=jnp.float32)
        hidden = jax.nn.silu(preact).astype(jnp.bfloat16)
        summed = jnp.zeros((2 * steps_len, D), jnp.float32)
        for index in range(N_HEAD):
            piece = jnp.dot(hidden[:, index * group:(index + 1) * group], second[:, index * group:(index + 1) * group].T, preferred_element_type=jnp.float32).astype(jnp.bfloat16)
            piece = lax.optimization_barrier(piece)
            summed = summed + piece.astype(jnp.float32)
        recalled = summed[:steps_len].astype(jnp.bfloat16)
        errors = (summed[steps_len:] - values.astype(jnp.float32)).astype(jnp.bfloat16)

        def shaped(array):
            return array.reshape(N_SEQ, TOK_DEV, HEADS, HEAD_DIM)

        out_heads = lax.map(lambda parts: attend_segment(parts, persist_keys, persist_values), (shaped(query), shaped(keys), shaped(values), shaped(recalled)))
        results.append(out_heads.reshape(steps_len, D))
        rate = lr_scale * jax.nn.sigmoid(jnp.dot(inputs.astype(jnp.float32), rate_weight, precision=lax.Precision.HIGHEST))
        weight = rate * jnp.exp(-tail[block])
        key_pre = preact[steps_len:]
        key_hidden = hidden[steps_len:]
        sigm = jax.nn.sigmoid(key_pre)
        back = jnp.dot(errors, second, preferred_element_type=jnp.float32)
        dpre = back * sigm * (1.0 + key_pre * (1.0 - sigm))
        wdz = (weight[:, None] * dpre).astype(jnp.bfloat16)
        whid = (weight[:, None] * key_hidden.astype(jnp.float32)).astype(jnp.bfloat16)
        grad_first = jnp.dot(keys.T, wdz, preferred_element_type=jnp.float32)
        grad_second = jnp.dot(errors.T, whid, preferred_element_type=jnp.float32)
        grad = jnp.stack([grad_first, grad_second], axis=1)
        momentum = momentum_decay[block] * momentum - grad
        memory = (1.0 - forget_share[block]) * memory + momentum
    return jnp.stack(results, axis=0), memory, momentum
```

```python
import functools

import jax
import jax.numpy as jnp
from jax import lax
from jax.experimental import pallas as pl
from jax.experimental.pallas import tpu as pltpu
from jax.sharding import PartitionSpec as P

HEAD_DIM = 128
MESH = pl.DeviceIdType.MESH
VMEM_LIMIT = 67043328
F32, BF16 = jnp.float32, jnp.bfloat16


def remote(src, dst, send_sem, recv_sem, where):
    return pltpu.make_async_remote_copy(
        src_ref=src,
        dst_ref=dst,
        send_sem=send_sem,
        recv_sem=recv_sem,
        device_id=where,
        device_id_type=MESH,
    )


def dot(a, b):
    return jnp.dot(a, b, preferred_element_type=F32)


def dot_nt(a, b):
    return lax.dot_general(a, b, (((1,), (1,)), ((), ())), preferred_element_type=F32)


def dot_tn(a, b):
    return lax.dot_general(a, b, (((0,), (0,)), ((), ())), preferred_element_type=F32)


class Place:
    def __init__(self, n_seq, n_head):
        self.n_seq, self.n_head = n_seq, n_head
        self.length = n_seq // 4
        self.seq, self.head = lax.axis_index("seq"), lax.axis_index("head")
        self.line = self.seq // 4
        self.side = (self.seq // 2) % 2
        self.core = self.seq % 2

    def at(self, line, side, core):
        return {"seq": (line * 2 + side) * 2 + core}

    def order(self, i):
        left, right = self.line, self.length - 1 - self.line
        both = jnp.minimum(left, right)
        paired = i <= 2 * both
        step = jnp.where(paired, (i + 1) // 2, i - both)
        to_left = jnp.where(paired, i % 2 == 1, left > right)
        return jnp.where(to_left, self.line - step, self.line + step)

    def peers(self):
        return [{"head": (self.head + by) % self.n_head} for by in range(1, self.n_head)]


def rows_loop(total, step, body):
    @pl.loop(0, total // step)
    def _(i):
        body(pl.ds(pl.multiple_of(i * step, step), step))


def forward_kernel(
    n_seq, n_head, lr_scale,
    tok, qkv, own, rate_w, forget,
    xx_out, yy_out, q_out, v_out, recall_out,
    W, wbuf, keys, query, values, zk, zz, hk, hq, wh, errs, err, recall, weight, frb,
    w_send, w_recv, f_send, f_recv, k_send, k_recv, e_send, e_recv, qkv_sem, out_sem,
):
    me = Place(n_seq, n_head)
    L, line, side, core, head = me.length, me.line, me.side, me.core, me.head
    chips = n_seq // 2
    count, width = tok.shape
    R, H = own.shape[1], own.shape[2]
    wide = 2 * R
    FB = values.shape[0]
    base = head * FB
    peers = me.peers()

    loads = [pltpu.make_async_copy(qkv.at[k], wbuf.at[s], qkv_sem.at[k]) for k, s in ((1, 0), (0, 1), (2, 0))]
    loads[0].start()
    loads[1].start()

    barrier = pltpu.get_barrier_semaphore()
    for by in range(1, n_seq):
        pl.semaphore_signal(barrier, inc=1, device_id={"seq": (me.seq + by) % n_seq}, device_id_type=MESH)
    for peer in peers:
        pl.semaphore_signal(barrier, inc=1, device_id=peer, device_id_type=MESH)
    pl.semaphore_wait(barrier, n_seq - 1 + n_head - 1)

    def block(w, l, m, c):
        return W.at[w, l * 2 + m, pl.ds(pl.multiple_of(c * R, R), R), :]

    def copy(w, l, m, c, way, src=None):
        where = (
            me.at(line + 1, side, core),
            me.at(line - 1, side, core),
            me.at(line, 1 - side, core),
            me.at(line, side, 1 - core),
        )[way]
        dst = block(w, l, m, c)
        chip = l * 2 + m
        return remote(dst if src is None else src, dst, w_send.at[w, way, chip], w_recv.at[w, chip * 2 + c], where)

    def spread(w, l, src, act):
        @pl.when((l <= line) & (line < L - 1))
        def _():
            act(copy(w, l, side, core, 0, src))

        @pl.when((l >= line) & (line > 0))
        def _():
            act(copy(w, l, side, core, 1, src))

        act(copy(w, l, side, core, 2, src))
        act(copy(w, l, side, core, 3, src))

    def start_own(w):
        spread(w, line, own.at[w], lambda c: c.start())
        W[w, line * 2 + side, pl.ds(pl.multiple_of(core * R, R), R), :] = own[w]

    def arrived(w, l, m, c):
        copy(w, l, m, c, 2).wait_recv()

    start_own(0)
    fcopies = []
    for by in range(1, n_seq):
        fcopies.append(
            remote(forget, frb.at[me.seq], f_send.at[by], f_recv.at[me.seq], {"seq": (me.seq + by) % n_seq})
        )
    for c in fcopies:
        c.start()
    frb[me.seq] = forget[...]

    def xcopy(which, buf, b, p):
        return remote(
            buf.at[base + b], buf.at[base + b], k_send.at[which, p, b], k_recv.at[which, base + b], peers[p]
        )

    def project(slot, b):
        cols = pl.ds(pl.multiple_of(b * wide, wide), wide)
        return dot(tok[...], wbuf[slot, :, cols]).astype(BF16)

    for which, (buf, slot) in enumerate(((keys, 0), (query, 1))):
        loads[which].wait()

        @pl.loop(0, FB)
        def _(b):
            buf[base + b] = project(slot, b)
            for p in range(n_head - 1):
                xcopy(which, buf, b, p).start()

        if which == 0:
            loads[2].start()
    loads[2].wait()

    @pl.loop(0, FB)
    def _(b):
        values[b] = project(0, b)

    for by in range(1, n_seq):
        other = (me.seq + by) % n_seq
        remote(forget, frb.at[other], f_send.at[by], f_recv.at[other], {"seq": other}).wait_recv()
    totals = jnp.sum(frb[...], axis=2, keepdims=True)
    which_seq = lax.broadcasted_iota(jnp.int32, totals.shape, 0)
    later = jnp.sum(jnp.where(which_seq > me.seq, totals, 0.0), axis=(0, 1, 2), keepdims=True)[0]

    def weigh(rows, start):
        x = tok[rows, :].astype(F32)
        rate = jnp.sum(x * rate_w[...], axis=1, keepdims=True)
        n = x.shape[0]
        t = lax.broadcasted_iota(jnp.int32, (n, count), 0) + start
        u = lax.broadcasted_iota(jnp.int32, (n, count), 1)
        tail = jnp.sum(jnp.where(u > t, forget[...], 0.0), axis=1, keepdims=True) + later
        weight[rows, :] = lr_scale * jax.nn.sigmoid(rate) * jnp.exp(-tail)

    @pl.loop(0, count // 32)
    def _(i):
        weigh(pl.ds(pl.multiple_of(i * 32, 32), 32), i * 32)

    def receive(w, i):
        @pl.when((i > 0) & (i < L))
        def _():
            l = me.order(i)
            arrived(w, l, side, core)
            spread(w, l, None, lambda c: c.start())

    def side_ready(w, l, mm):
        m = jnp.where(mm == 0, side, 1 - side)

        @pl.when(mm == 1)
        def _():
            arrived(w, l, m, core)
            copy(w, l, m, core, 3).start()

        arrived(w, l, m, 1 - core)
        return l * 2 + m

    zk[...] = jnp.zeros_like(zk)

    def keys_ready(which, buf, j):
        @pl.when((j < base) | (j >= base + FB))
        def _():
            remote(buf.at[j], buf.at[j], k_send.at[which, 0, 0], k_recv.at[which, j], peers[0]).wait_recv()

    @pl.loop(0, L + 1)
    def _(i):
        receive(0, i)

        @pl.when(i == L - 1)
        def _():
            start_own(1)

        @pl.when(i > 0)
        def _():
            l = me.order(i - 1)

            @pl.loop(0, 2)
            def _(mm):
                j = side_ready(0, l, mm)
                keys_ready(0, keys, j)
                zk[...] += dot(keys[j], W[0, j])

    keys_out = pltpu.make_async_copy(keys, xx_out.at[0], out_sem.at[0])
    keys_out.start()
    values_out = pltpu.make_async_copy(values, v_out, out_sem.at[1])
    values_out.start()
    query_out = pltpu.make_async_copy(query.at[pl.ds(base, FB)], q_out, out_sem.at[2])
    query_out.start()

    def hide(rows):
        hid = jax.nn.silu(zk[rows, :]).astype(BF16)
        hk[rows, :] = hid
        wh[rows, :] = (weight[rows, :] * hid.astype(F32)).astype(BF16)

    rows_loop(count, 16, hide)
    wh_out = pltpu.make_async_copy(wh, yy_out.at[1], out_sem.at[3])
    wh_out.start()

    def ecopy(j, p):
        return remote(errs.at[head, j], errs.at[head, j], e_send.at[p, j], e_recv.at[head, j], peers[p])

    @pl.loop(0, L + 2)
    def _(i):
        receive(1, i)

        @pl.when(i == 1)
        def _():
            @pl.loop(0, chips)
            def _(j):
                keys_ready(1, query, j)

            zz[...] = jnp.zeros_like(zz)

            @pl.loop(0, chips)
            def _(j):
                zz[...] += dot(query[j], W[0, j])

            def hide_query(rows):
                hq[rows, :] = jax.nn.silu(zz[rows, :]).astype(BF16)

            rows_loop(count, 16, hide_query)
            zz[...] = jnp.zeros_like(zz)

        @pl.when((i > 0) & (i <= L))
        def _():
            l = me.order(i - 1)

            @pl.loop(0, 2)
            def _(mm):
                j = side_ready(1, l, mm)
                part = dot_nt(hk[...], W[1, j])
                mine = (j >= base) & (j < base + FB)

                @pl.when(mine)
                def _():
                    errs[head, j] = (part - values[j - base].astype(F32)).astype(BF16)

                @pl.when(jnp.logical_not(mine))
                def _():
                    errs[head, j] = part.astype(BF16)

                for p in range(n_head - 1):
                    ecopy(j, p).start()
                recall[j] = dot_nt(hq[...], W[1, j]).astype(BF16)

        @pl.when(i > 1)
        def _():
            l = me.order(i - 2)

            @pl.loop(0, 2)
            def _(mm):
                j = l * 2 + jnp.where(mm == 0, side, 1 - side)
                for by in range(1, n_head):
                    other = (head + by) % n_head
                    remote(
                        errs.at[other, j], errs.at[other, j], e_send.at[0, j], e_recv.at[other, j], peers[0]
                    ).wait_recv()
                total = errs[0, j].astype(F32)
                for p in range(1, n_head):
                    total = total + errs[p, j].astype(F32)
                err[j] = total.astype(BF16)
                zz[...] += dot(err[j], W[1, j])

    err_out = pltpu.make_async_copy(err, xx_out.at[1], out_sem.at[4])
    err_out.start()
    recall_copy = pltpu.make_async_copy(recall, recall_out, out_sem.at[5])
    recall_copy.start()

    def pull(rows):
        z = zk[rows, :]
        s = jax.nn.sigmoid(z)
        dz = zz[rows, :] * s * (1.0 + z * (1.0 - s))
        hk[rows, :] = (weight[rows, :] * dz).astype(BF16)

    rows_loop(count, 16, pull)
    wdz_out = pltpu.make_async_copy(hk, yy_out.at[0], out_sem.at[6])
    wdz_out.start()

    for c in fcopies:
        c.wait_send()

    @pl.loop(0, FB)
    def _(b):
        for which, buf in enumerate((keys, query)):
            for p in range(n_head - 1):
                xcopy(which, buf, b, p).wait_send()

    @pl.loop(0, chips)
    def _(j):
        for p in range(n_head - 1):
            ecopy(j, p).wait_send()

    @pl.loop(0, L)
    def _(l):
        for w in range(2):
            spread(w, l, None, lambda c: c.wait_send())
            copy(w, l, 1 - side, core, 3).wait_send()

    for c in (keys_out, values_out, query_out, wh_out, err_out, recall_copy, wdz_out):
        c.wait()


def forward(tok, qkv, own, rate_w, forget, n_seq, n_head, lr_scale):
    count, width = tok.shape
    _, R, H = own.shape
    F = qkv.shape[2]
    chips, wide = n_seq // 2, 2 * R
    FB = F // wide
    assert n_seq % 4 == 0 and n_seq >= 8 and FB * wide == F and chips * wide == width
    anywhere = pl.BlockSpec(memory_space=pl.ANY)
    vmem = pl.BlockSpec(memory_space=pltpu.VMEM)
    S = jax.ShapeDtypeStruct
    dma = pltpu.SemaphoreType.DMA
    return pl.pallas_call(
        functools.partial(forward_kernel, n_seq, n_head, lr_scale),
        out_shape=(
            S((2, chips, count, wide), BF16),
            S((2, count, H), BF16),
            S((FB, count, wide), BF16),
            S((FB, count, wide), BF16),
            S((chips, count, wide), BF16),
        ),
        in_specs=[vmem, anywhere, vmem, vmem, vmem],
        out_specs=(anywhere,) * 5,
        scratch_shapes=[
            pltpu.VMEM((2, chips, wide, H), BF16),
            pltpu.VMEM((2, width, F), BF16),
            pltpu.VMEM((chips, count, wide), BF16),
            pltpu.VMEM((chips, count, wide), BF16),
            pltpu.VMEM((FB, count, wide), BF16),
            pltpu.VMEM((count, H), F32),
            pltpu.VMEM((count, H), F32),
            pltpu.VMEM((count, H), BF16),
            pltpu.VMEM((count, H), BF16),
            pltpu.VMEM((count, H), BF16),
            pltpu.VMEM((n_head, chips, count, wide), BF16),
            pltpu.VMEM((chips, count, wide), BF16),
            pltpu.VMEM((chips, count, wide), BF16),
            pltpu.VMEM((count, 1), F32),
            pltpu.VMEM((n_seq, 1, count), F32),
            dma((2, 4, chips)),
            dma((2, n_seq)),
            dma((n_seq,)),
            dma((n_seq,)),
            dma((2, max(n_head - 1, 1), FB)),
            dma((2, chips)),
            dma((max(n_head - 1, 1), chips)),
            dma((n_head, chips)),
            dma((3,)),
            dma((7,)),
        ],
        compiler_params=pltpu.CompilerParams(
            collective_id=0, has_side_effects=True, vmem_limit_bytes=VMEM_LIMIT
        ),
    )(tok, qkv, own, rate_w, forget)


def backward_kernel(
    n_seq, n_head,
    xx_in, yy_in, q_in, v_in, recall_in, persist,
    grad, attended,
    xx, yy, query, values, recall, got, recalled, G, from_core, from_side, from_left, from_right, acc,
    c_send, c_recv, s_send, s_recv, z_send, l_recv, r_recv, x_send, x_recv, in_sem,
):
    me = Place(n_seq, n_head)
    L, line, side, core, head = me.length, me.line, me.side, me.core, me.head
    count, wide = xx.shape[2], xx.shape[3]
    R, H = acc.shape
    FB = query.shape[0]
    base = head * FB
    peers = me.peers()

    pairs = (
        (recall_in, recall), (xx_in.at[1], xx.at[1]), (yy_in.at[1], yy.at[1]), (xx_in.at[0], xx.at[0]),
        (yy_in.at[0], yy.at[0]), (q_in, query), (v_in, values),
    )
    loads = [pltpu.make_async_copy(a, b, in_sem.at[i]) for i, (a, b) in enumerate(pairs)]
    for c in loads:
        c.start()

    barrier = pltpu.get_barrier_semaphore()

    def greet(where):
        pl.semaphore_signal(barrier, inc=1, device_id=where, device_id_type=MESH)

    greet(me.at(line, side, 1 - core))
    greet(me.at(line, 1 - side, core))

    @pl.when(line > 0)
    def _():
        greet(me.at(line - 1, side, core))

    @pl.when(line < L - 1)
    def _():
        greet(me.at(line + 1, side, core))

    for peer in peers:
        greet(peer)
    ends = jnp.where(line > 0, 1, 0) + jnp.where(line < L - 1, 1, 0)
    pl.semaphore_wait(barrier, 2 + n_head - 1 + ends)

    def rcopy(b, p):
        there = peers[p]["head"] * FB
        return remote(recall.at[there + b], got.at[head, b], x_send.at[p, b], x_recv.at[head, b], peers[p])

    loads[0].wait()

    @pl.loop(0, FB)
    def _(b):
        for p in range(n_head - 1):
            rcopy(b, p).start()

    for c in loads[1:5]:
        c.wait()

    mine = pl.ds(pl.multiple_of(core * R, R), R)
    theirs = pl.ds(pl.multiple_of((1 - core) * R, R), R)

    def core_copy(w, j):
        return remote(
            G.at[w, j, theirs, :], from_core.at[w, j], c_send.at[w, j], c_recv.at[w, j],
            me.at(line, side, 1 - core),
        )

    def side_copy(w, l):
        return remote(
            G.at[w, l * 2 + 1 - side, mine, :], from_side.at[w, l], s_send.at[w, l], s_recv.at[w, l],
            me.at(line, 1 - side, core),
        )

    def right_copy(w, l):
        return remote(
            G.at[w, l * 2 + side, mine, :], from_left.at[w, l], z_send.at[w, l], l_recv.at[w, l],
            me.at(line + 1, side, core),
        )

    def left_copy(w, l):
        return remote(
            G.at[w, l * 2 + side, mine, :], from_right.at[w, l], z_send.at[w, l], r_recv.at[w, l],
            me.at(line - 1, side, core),
        )

    def partial(w, j):
        G[w, j] = dot_tn(xx[w, j], yy[w]).astype(BF16)
        core_copy(w, j).start()

    @pl.loop(0, 2 * L + 1)
    def _(n):
        @pl.when(n < 2 * L)
        def _():
            partial(1 - n // L, me.order(L - 1 - n % L) * 2 + 1 - side)

        @pl.when(n > 0)
        def _():
            w, l = 1 - (n - 1) // L, me.order(L - 1 - (n - 1) % L)
            j = l * 2 + 1 - side
            core_copy(w, j).wait_recv()
            both = G[w, j, mine, :].astype(F32) + from_core[w, j].astype(F32)
            G[w, j, mine, :] = both.astype(BF16)
            side_copy(w, l).start()

    heads_here = FB * wide // HEAD_DIM
    per = wide // HEAD_DIM
    chunk = count // 2
    scale = HEAD_DIM ** (-0.5)
    persist_count = persist.shape[1]

    def attend(n):
        b = n // per
        cols = pl.ds(pl.multiple_of((n % per) * HEAD_DIM, HEAD_DIM), HEAD_DIM)
        flat = pl.ds(pl.multiple_of(n * HEAD_DIM, HEAD_DIM), HEAD_DIM)
        for part in range(2):
            seen = (part + 1) * chunk
            q = query[b, pl.ds(part * chunk, chunk), cols]
            row = lax.broadcasted_iota(jnp.int32, (chunk, seen), 0) + part * chunk
            visible = lax.broadcasted_iota(jnp.int32, (chunk, seen), 1) <= row
            rec = recalled[b, pl.ds(0, seen), cols]
            key = xx[0, base + b, pl.ds(0, seen), cols]
            val = values[b, pl.ds(0, seen), cols]
            s0 = dot_nt(q, persist[0, :, flat]) * scale
            s1 = jnp.where(visible, dot_nt(q, rec) * scale, -1e30)
            s2 = jnp.where(visible, dot_nt(q, key) * scale, -1e30)
            top = jnp.maximum(
                jnp.max(s0, axis=1, keepdims=True),
                jnp.maximum(jnp.max(s1, axis=1, keepdims=True), jnp.max(s2, axis=1, keepdims=True)),
            )
            e0, e1, e2 = jnp.exp(s0 - top), jnp.exp(s1 - top), jnp.exp(s2 - top)
            norm = 1.0 / (
                jnp.sum(e0, axis=1, keepdims=True)
                + jnp.sum(e1, axis=1, keepdims=True)
                + jnp.sum(e2, axis=1, keepdims=True)
            )
            out = dot((e0 * norm).astype(BF16), persist[1, :, flat])
            out = out + dot((e1 * norm).astype(BF16), rec)
            out = out + dot((e2 * norm).astype(BF16), val)
            attended[pl.ds(part * chunk, chunk), flat] = out.astype(BF16)

    each = -(-heads_here // (2 * L))

    @pl.loop(0, 2 * L)
    def _(n):
        w, l = 1 - n // L, me.order(L - 1 - n % L)
        j = l * 2 + side
        partial(w, j)
        core_copy(w, j).wait_recv()
        remote(
            from_side.at[w, l], from_side.at[w, l], s_send.at[w, l], s_recv.at[w, l], me.at(line, 1 - side, core)
        ).wait_recv()
        acc[...] = G[w, j, mine, :].astype(F32) + from_core[w, j].astype(F32) + from_side[w, l].astype(F32)

        @pl.when((l >= line) & (line > 0))
        def _():
            remote(
                from_left.at[w, l], from_left.at[w, l], z_send.at[w, l], l_recv.at[w, l],
                me.at(line - 1, side, core),
            ).wait_recv()
            acc[...] += from_left[w, l].astype(F32)

        @pl.when((l <= line) & (line < L - 1))
        def _():
            remote(
                from_right.at[w, l], from_right.at[w, l], z_send.at[w, l], r_recv.at[w, l],
                me.at(line + 1, side, core),
            ).wait_recv()
            acc[...] += from_right[w, l].astype(F32)

        @pl.when(l == line)
        def _():
            grad[w] = acc[...]

        @pl.when(l != line)
        def _():
            G[w, j, mine, :] = acc[...].astype(BF16)

        @pl.when(l > line)
        def _():
            right_copy(w, l).start()

        @pl.when(l < line)
        def _():
            left_copy(w, l).start()

        @pl.when(n == 0)
        def _():
            loads[5].wait()
            loads[6].wait()

            @pl.loop(0, FB)
            def _(b):
                total = recall[base + b].astype(F32)
                for by in range(1, n_head):
                    other = (head + by) % n_head
                    remote(
                        got.at[other, b], got.at[other, b], x_send.at[0, b], x_recv.at[other, b], peers[0]
                    ).wait_recv()
                    total = total + got[other, b].astype(F32)
                recalled[b] = total.astype(BF16)

        for k in range(each):
            @pl.when(n * each + k < heads_here)
            def _():
                attend(n * each + k)

    @pl.loop(0, FB)
    def _(b):
        for p in range(n_head - 1):
            rcopy(b, p).wait_send()

    @pl.loop(0, L)
    def _(l):
        for w in range(2):
            core_copy(w, l * 2).wait_send()
            core_copy(w, l * 2 + 1).wait_send()
            side_copy(w, l).wait_send()

            @pl.when(l > line)
            def _():
                right_copy(w, l).wait_send()

            @pl.when(l < line)
            def _():
                left_copy(w, l).wait_send()


def backward(xx, yy, query, values, recall, persist, n_seq, n_head, R):
    _, chips, count, wide = xx.shape
    H, FB = yy.shape[2], query.shape[0]
    L = n_seq // 4
    anywhere = pl.BlockSpec(memory_space=pl.ANY)
    vmem = pl.BlockSpec(memory_space=pltpu.VMEM)
    S = jax.ShapeDtypeStruct
    dma = pltpu.SemaphoreType.DMA
    return pl.pallas_call(
        functools.partial(backward_kernel, n_seq, n_head),
        out_shape=(S((2, R, H), F32), S((count, FB * wide), BF16)),
        in_specs=[anywhere] * 5 + [vmem],
        out_specs=(vmem, vmem),
        scratch_shapes=[
            pltpu.VMEM((2, chips, count, wide), BF16),
            pltpu.VMEM((2, count, H), BF16),
            pltpu.VMEM((FB, count, wide), BF16),
            pltpu.VMEM((FB, count, wide), BF16),
            pltpu.VMEM((chips, count, wide), BF16),
            pltpu.VMEM((n_head, FB, count, wide), BF16),
            pltpu.VMEM((FB, count, wide), BF16),
            pltpu.VMEM((2, chips, wide, H), BF16),
            pltpu.VMEM((2, chips, R, H), BF16),
            pltpu.VMEM((2, L, R, H), BF16),
            pltpu.VMEM((2, L, R, H), BF16),
            pltpu.VMEM((2, L, R, H), BF16),
            pltpu.VMEM((R, H), F32),
            dma((2, chips)),
            dma((2, chips)),
            dma((2, L)),
            dma((2, L)),
            dma((2, L)),
            dma((2, L)),
            dma((2, L)),
            dma((max(n_head - 1, 1), FB)),
            dma((n_head, FB)),
            dma((7,)),
        ],
        compiler_params=pltpu.CompilerParams(
            collective_id=1, has_side_effects=True, vmem_limit_bytes=VMEM_LIMIT
        ),
    )(xx, yy, query, values, recall, persist)


def on_device(
    tokens, qkv_weight, persistent, rate_weight, forget_rate, momentum_decay, forget_share, memory, momentum
):
    n_seq, n_head = lax.axis_size("seq"), lax.axis_size("head")
    seg_len, width = tokens.shape[1], tokens.shape[2]
    lr_scale = 2.0 / (width * n_seq * seg_len) ** 0.5
    own = jnp.transpose(memory.astype(BF16), (1, 0, 2))
    qkv = jnp.transpose(qkv_weight, (1, 0, 2))
    xx, yy, query, values, recall = forward(
        tokens[0], qkv, own, rate_weight[None], forget_rate, n_seq, n_head, lr_scale
    )
    grad, attended = backward(xx, yy, query, values, recall, persistent, n_seq, n_head, memory.shape[0])
    grad = jnp.transpose(grad, (1, 0, 2))
    momentum = momentum_decay[0] * momentum - grad
    memory = (1.0 - forget_share[0]) * memory + momentum
    return (attended[None], memory, momentum)


def solution(mesh):
    placed = (
        P(None, "seq", None),
        P(None, None, "head"),
        P(None, None, "head"),
        P(),
        P(None, "seq"),
        P(),
        P(),
        P("seq", None, "head"),
        P("seq", None, "head"),
    )
    return jax.shard_map(
        on_device,
        mesh=mesh,
        in_specs=placed,
        out_specs=(P(None, "seq", "head"), P("seq", None, "head"), P("seq", None, "head")),
        check_vma=False,
    )
```

```python
import functools

import jax
import jax.numpy as jnp
from jax import lax
from jax.experimental import pallas as pl
from jax.experimental.pallas import tpu as pltpu
from jax.sharding import PartitionSpec as P

HEAD_DIM = 128
LANES = 128
MESH = pl.DeviceIdType.MESH
VMEM_LIMIT = 67043328
PIECES = 2
EARLY = 2
F32, BF16 = jnp.float32, jnp.bfloat16


def remote(src, dst, send_sem, recv_sem, where):
    return pltpu.make_async_remote_copy(
        src_ref=src,
        dst_ref=dst,
        send_sem=send_sem,
        recv_sem=recv_sem,
        device_id=where,
        device_id_type=MESH,
    )


def dot(a, b):
    return jnp.dot(a, b, preferred_element_type=F32)


def dot_nt(a, b):
    return lax.dot_general(a, b, (((1,), (1,)), ((), ())), preferred_element_type=F32)


def dot_tn(a, b):
    return lax.dot_general(a, b, (((0,), (0,)), ((), ())), preferred_element_type=F32)


class Place:
    def __init__(self, n_seq, n_head):
        self.n_seq, self.n_head = n_seq, n_head
        self.length = n_seq // 4
        self.seq, self.head = lax.axis_index("seq"), lax.axis_index("head")
        self.line = self.seq // 4
        self.side = (self.seq // 2) % 2
        self.core = self.seq % 2

    def at(self, line, side, core):
        return {"seq": (line * 2 + side) * 2 + core}

    def order(self, i):
        left, right = self.line, self.length - 1 - self.line
        both = jnp.minimum(left, right)
        paired = i <= 2 * both
        step = jnp.where(paired, (i + 1) // 2, i - both)
        to_left = jnp.where(paired, i % 2 == 1, left > right)
        return jnp.where(to_left, self.line - step, self.line + step)

    def peers(self):
        return [{"head": (self.head + by) % self.n_head} for by in range(1, self.n_head)]


def rows_loop(total, step, body):
    @pl.loop(0, total // step)
    def _(i):
        body(pl.ds(pl.multiple_of(i * step, step), step))


def forward_kernel(
    n_seq, n_head, lr_scale,
    tok, qkv, memory, rate_w, forget,
    xx_out, yy_out, q_out, v_out, recall_out, g_out,
    staged, own, W, wbuf, keys, query, values, zk, zz, hk, hq, wh, errs, recall, weight, frb, G, from_core, from_side,
    w_send, w_recv, f_send, f_recv, k_send, k_recv, e_send, e_recv, qkv_sem, out_sem, block_sem, g_send, g_recv, mem_sem,
):
    me = Place(n_seq, n_head)
    L, line, side, core, head = me.length, me.line, me.side, me.core, me.head
    chips = n_seq // 2
    count, width = tok.shape
    R, H = own.shape[1:]
    wide = 2 * R
    FB = values.shape[0]
    base = head * FB
    peers = me.peers()

    memory_load = pltpu.make_async_copy(memory, staged, mem_sem)
    memory_load.start()
    loads = [pltpu.make_async_copy(qkv.at[k], wbuf.at[s], qkv_sem.at[k]) for k, s in ((1, 0), (0, 1), (2, 0))]
    loads[0].start()
    loads[1].start()

    barrier = pltpu.get_barrier_semaphore()
    for by in range(1, n_seq):
        pl.semaphore_signal(barrier, inc=1, device_id={"seq": (me.seq + by) % n_seq}, device_id_type=MESH)
    for peer in peers:
        pl.semaphore_signal(barrier, inc=1, device_id=peer, device_id_type=MESH)
    memory_load.wait()
    each = 2 * H // LANES
    for k in range(2):
        for tile in range(H // LANES):
            tiles = staged[pl.ds(tile * 2 + k, R, stride=each), :]
            own[k, :, tile * LANES : (tile + 1) * LANES] = tiles.astype(BF16)
    pl.semaphore_wait(barrier, n_seq - 1 + n_head - 1)

    piece = R // PIECES

    def block(w, l, m, c, p):
        return W.at[w, l * 2 + m, pl.ds(pl.multiple_of(c * R + p * piece, piece), piece), :]

    def copy(w, l, m, c, p, way, mine=False):
        where = (
            me.at(line + 1, side, core),
            me.at(line - 1, side, core),
            me.at(line, 1 - side, core),
            me.at(line, side, 1 - core),
        )[way]
        dst = block(w, l, m, c, p)
        src = own.at[w, pl.ds(pl.multiple_of(p * piece, piece), piece), :] if mine else dst
        chip = l * 2 + m
        return remote(src, dst, w_send.at[w, way, chip, p], w_recv.at[w, chip * 2 + c, p], where)

    def spread(w, l, p, act, ways=(0, 1, 2, 3), mine=False):
        if 0 in ways:

            @pl.when((l <= line) & (line < L - 1))
            def _():
                act(copy(w, l, side, core, p, 0, mine))

        if 1 in ways:

            @pl.when((l >= line) & (line > 0))
            def _():
                act(copy(w, l, side, core, p, 1, mine))

        for way in (2, 3):
            if way in ways:
                act(copy(w, l, side, core, p, way, mine))

    def start(c):
        c.start()

    def arrived(w, l, m, c, p):
        copy(w, l, m, c, p, 2).wait_recv()

    def start_own(w, ways):
        for p in range(PIECES):
            spread(w, line, p, start, ways, True)

    for p in range(PIECES):
        spread(0, line, p, start, (0, 1, 3), True)
    spread(0, line, 0, start, (2,), True)
    fcopies = []
    for by in range(1, n_seq):
        fcopies.append(
            remote(forget, frb.at[me.seq], f_send.at[by], f_recv.at[me.seq], {"seq": (me.seq + by) % n_seq})
        )
    for c in fcopies:
        c.start()
    frb[me.seq] = forget[...]

    def xcopy(which, buf, b, p):
        return remote(
            buf.at[base + b], buf.at[base + b], k_send.at[which, p, b], k_recv.at[which, base + b], peers[p]
        )

    def project(slot, b):
        cols = pl.ds(pl.multiple_of(b * wide, wide), wide)
        return dot(tok[...], wbuf[slot, :, cols]).astype(BF16)

    def project_shared(which, buf, slot):
        loads[which].wait()

        @pl.loop(0, FB)
        def _(b):
            buf[base + b] = project(slot, b)
            for p in range(n_head - 1):
                xcopy(which, buf, b, p).start()

    def project_values():
        loads[2].wait()

        @pl.loop(0, FB)
        def _(b):
            values[b] = project(0, b)

    def weigh(rows, start_row, later):
        x = tok[rows, :].astype(F32)
        rate = jnp.sum(x * rate_w[...], axis=1, keepdims=True)
        n = x.shape[0]
        t = lax.broadcasted_iota(jnp.int32, (n, count), 0) + start_row
        u = lax.broadcasted_iota(jnp.int32, (n, count), 1)
        tail = jnp.sum(jnp.where(u > t, forget[...], 0.0), axis=1, keepdims=True) + later
        weight[rows, :] = lr_scale * jax.nn.sigmoid(rate) * jnp.exp(-tail)

    def weigh_all():
        for by in range(1, n_seq):
            other = (me.seq + by) % n_seq
            remote(forget, frb.at[other], f_send.at[by], f_recv.at[other], {"seq": other}).wait_recv()
        totals = jnp.sum(frb[...], axis=2, keepdims=True)
        which_seq = lax.broadcasted_iota(jnp.int32, totals.shape, 0)
        later = jnp.sum(jnp.where(which_seq > me.seq, totals, 0.0), axis=(0, 1, 2), keepdims=True)[0]

        @pl.loop(0, count // 32)
        def _(i):
            weigh(pl.ds(pl.multiple_of(i * 32, 32), 32), i * 32, later)

    for w in range(2):
        W[w, line * 2 + side, pl.ds(pl.multiple_of(core * R, R), R), :] = own[w]
    zk[...] = jnp.zeros_like(zk)
    right = L - 1 - line

    def keys_ready(which, buf, j):
        @pl.when((j < base) | (j >= base + FB))
        def _():
            remote(buf.at[j], buf.at[j], k_send.at[which, 0, 0], k_recv.at[which, j], peers[0]).wait_recv()

    def chip(l, mm):
        return l * 2 + jnp.where(mm == 0, side, 1 - side)

    def other_core(w, l, mm):
        for p in range(PIECES):
            arrived(w, l, jnp.where(mm == 0, side, 1 - side), 1 - core, p)

    def ecopy(j, p):
        return remote(errs.at[head, j], errs.at[head, j], e_send.at[p, j], e_recv.at[head, j], peers[p])

    def move(k):
        def come(away, step, ways):
            each = away * PIECES

            @pl.when((k > 0) & (k <= 2 * each))
            def _():
                at = k - 1
                w = jnp.where(at >= each, 1, 0)
                at = at - w * each
                l = line + step * (1 + at // PIECES)
                arrived(w, l, side, core, at % PIECES)
                spread(w, l, at % PIECES, start, ways)

            @pl.when(k == each)
            def _():
                start_own(1, ways[:1])

        come(line, -1, (0, 3))
        come(right, 1, (1, 3))

        @pl.when(k == 1)
        def _():
            start_own(1, (3,))

        total = 2 * L * PIECES

        def entry(n):
            return n // (L * PIECES), me.order(n // PIECES % L), n % PIECES

        half = L * PIECES
        first = k + jnp.where(k < half, 1, 2)
        end = jnp.minimum(k + jnp.where(k < half - 1, 2, 3), total)

        @pl.loop(first, end)
        def _(n):
            w, l, p = entry(n)

            @pl.when(l == line)
            def _():
                spread(w, l, p, start, (2,), True)

            @pl.when(l != line)
            def _():
                spread(w, l, p, start, (2,))

        @pl.when((k > 0) & (k <= total))
        def _():
            w, l, p = entry(k - 1)
            arrived(w, l, 1 - side, core, p)
            copy(w, l, 1 - side, core, p, 3).start()

    def hide(rows):
        z = zk[rows, :]
        s = jax.nn.sigmoid(z)
        hid = (z * s).astype(BF16)
        hk[rows, :] = hid
        wh[rows, :] = (weight[rows, :] * hid.astype(F32)).astype(BF16)
        zk[rows, :] = weight[rows, :] * (s * (1.0 + z * (1.0 - s)))

    def hide_query(rows):
        hq[rows, :] = jax.nn.silu(zz[rows, :]).astype(BF16)

    keys_out = pltpu.make_async_copy(keys, xx_out.at[0], out_sem.at[0])
    values_out = pltpu.make_async_copy(values, v_out, out_sem.at[1])
    query_out = pltpu.make_async_copy(query.at[pl.ds(base, FB)], q_out, out_sem.at[2])
    wh_out = pltpu.make_async_copy(wh, yy_out.at[1], out_sem.at[3])

    def err_copy(j):
        return pltpu.make_async_copy(errs.at[head, j], xx_out.at[1, j], block_sem.at[0, j])

    def recall_copy(j):
        return pltpu.make_async_copy(recall.at[j], recall_out.at[j], block_sem.at[1, j])

    def add_first(i):
        @pl.loop(0, 2)
        def _(mm):
            l = me.order(i)
            other_core(0, l, mm)
            j = chip(l, mm)
            keys_ready(0, keys, j)
            zk[...] += dot(keys[j], W[0, j])

    def make_error(i, mm):
        @pl.when((i >= 0) & (i < L))
        def _():
            l = me.order(i)
            other_core(1, l, mm)
            j = chip(l, mm)
            part = dot_nt(hk[...], W[1, j])
            mine = (j >= base) & (j < base + FB)

            @pl.when(mine)
            def _():
                errs[head, j] = (part - values[j - base].astype(F32)).astype(BF16)

            @pl.when(jnp.logical_not(mine))
            def _():
                errs[head, j] = part.astype(BF16)

            for p in range(n_head - 1):
                ecopy(j, p).start()

    def make_recall(i):
        @pl.loop(0, 2)
        def _(mm):
            j = chip(me.order(i), mm)
            recall[j] = dot_nt(hq[...], W[1, j]).astype(BF16)
            recall_copy(j).start()

    def pull_error(i, mm):
        @pl.when((i >= 0) & (i < L))
        def _():
            j = chip(me.order(i), mm)
            for by in range(1, n_head):
                other = (head + by) % n_head
                remote(
                    errs.at[other, j], errs.at[other, j], e_send.at[0, j], e_recv.at[other, j], peers[0]
                ).wait_recv()
            total = errs[0, j].astype(F32)
            for p in range(1, n_head):
                total = total + errs[p, j].astype(F32)
            for p in range(n_head - 1):
                ecopy(j, p).wait_send()
            errs[head, j] = total.astype(BF16)
            err_copy(j).start()
            zz[...] += dot(errs[head, j], W[1, j])

    mine = pl.ds(pl.multiple_of(core * R, R), R)
    theirs = pl.ds(pl.multiple_of((1 - core) * R, R), R)

    def early_core(i):
        return remote(
            G.at[i, theirs, :], from_core.at[i], g_send.at[0, i], g_recv.at[0, i], me.at(line, side, 1 - core)
        )

    def early_side(i):
        return remote(
            G.at[i, mine, :], from_side.at[i], g_send.at[1, i], g_recv.at[1, i], me.at(line, 1 - side, core)
        )

    def early_partial(i):
        G[i] = dot_tn(errs[head, chip(me.order(i), 1)], wh[...]).astype(BF16)
        early_core(i).start()

    def early_on(i):
        early_core(i).wait_recv()
        G[i, mine, :] = (G[i, mine, :].astype(F32) + from_core[i].astype(F32)).astype(BF16)
        early_side(i).start()

    def add_query(low, high):
        @pl.loop(low, high)
        def _(j):
            keys_ready(1, query, j)
            zz[...] += dot(query[j], W[0, j])

    @pl.loop(0, PIECES * (2 * L + 1) + 1)
    def _(k):
        move(k)
        slot = k // PIECES
        even = k % PIECES == 0
        last = k % PIECES == PIECES - 1

        @pl.when(k == 0)
        def _():
            project_shared(0, keys, 0)
            loads[2].start()

        @pl.when(k == 1)
        def _():
            project_shared(1, query, 1)

        @pl.when(k == PIECES)
        def _():
            project_values()

        @pl.when(k == PIECES + 1)
        def _():
            weigh_all()

        @pl.when(even & (slot > 0) & (slot <= L))
        def _():
            add_first(slot - 1)

        @pl.when(k == PIECES * L)
        def _():
            keys_out.start()
            rows_loop(count, 16, hide)
            wh_out.start()
            zz[...] = jnp.zeros_like(zz)

        @pl.when(even & (slot >= L) & (slot <= 2 * L))
        def _():
            @pl.loop(jnp.where(slot == L, -1, 0), 2)
            def _(nth):
                mm = jnp.maximum(nth, 0)
                make_error(slot - L + jnp.where(nth < 0, 0, 1 - 2 * mm), mm)

        @pl.when(k == PIECES * L + 1)
        def _():
            add_query(0, chips // 2)

        @pl.when(k == PIECES * (L + 1) + 1)
        def _():
            add_query(chips // 2, chips)
            rows_loop(count, 16, hide_query)
            zz[...] = jnp.zeros_like(zz)
            values_out.start()
            query_out.start()

        @pl.when(last & (slot > L) & (slot <= 2 * L))
        def _():
            make_recall(slot - L - 1)

        @pl.when((last & (slot > L)) | (k == PIECES * (2 * L + 1)))
        def _():
            @pl.loop(jnp.where(slot == L + 1, -1, 0), 2)
            def _(nth):
                mm = jnp.maximum(nth, 0)
                pull_error(slot - L - jnp.where(nth < 0, 1, 2 * mm), mm)

        @pl.when(even & (slot > 2 * L - 2) & (slot <= 2 * L - 2 + EARLY))
        def _():
            early_on(slot - 2 * L + 1)

        @pl.when(last & (slot > 2 * L - 3) & (slot <= 2 * L - 3 + EARLY))
        def _():
            early_partial(slot - 2 * L + 2)


    def pull(rows):
        hk[rows, :] = (zz[rows, :] * zk[rows, :]).astype(BF16)

    rows_loop(count, 16, pull)
    wdz_out = pltpu.make_async_copy(hk, yy_out.at[0], out_sem.at[4])
    wdz_out.start()
    early_out = []
    for i in range(EARLY):
        early_side(i).wait_recv()
        early_out.append(pltpu.make_async_copy(from_side.at[i], g_out.at[i], out_sem.at[5 + i]))
        early_out[i].start()

    for c in fcopies:
        c.wait_send()

    @pl.loop(0, FB)
    def _(b):
        for which, buf in enumerate((keys, query)):
            for p in range(n_head - 1):
                xcopy(which, buf, b, p).wait_send()

    @pl.loop(0, L)
    def _(l):
        for w in range(2):
            for p in range(PIECES):
                spread(w, l, p, lambda c: c.wait_send())
                copy(w, l, 1 - side, core, p, 3).wait_send()

    for i in range(EARLY):
        early_core(i).wait_send()
        early_side(i).wait_send()

    @pl.loop(0, chips)
    def _(j):
        err_copy(j).wait()
        recall_copy(j).wait()

    for c in (keys_out, values_out, query_out, wh_out, wdz_out, *early_out):
        c.wait()


def forward(tok, qkv, memory, rate_w, forget, R, H, n_seq, n_head, lr_scale):
    count, width = tok.shape
    F = qkv.shape[2]
    chips, wide = n_seq // 2, 2 * R
    FB = F // wide
    assert n_seq % 4 == 0 and n_seq >= 16 and FB * wide == F and chips * wide == width
    anywhere = pl.BlockSpec(memory_space=pl.ANY)
    vmem = pl.BlockSpec(memory_space=pltpu.VMEM)
    S = jax.ShapeDtypeStruct
    dma = pltpu.SemaphoreType.DMA
    return pl.pallas_call(
        functools.partial(forward_kernel, n_seq, n_head, lr_scale),
        out_shape=(
            S((2, chips, count, wide), BF16),
            S((2, count, H), BF16),
            S((FB, count, wide), BF16),
            S((FB, count, wide), BF16),
            S((chips, count, wide), BF16),
            S((EARLY, R, H), BF16),
        ),
        in_specs=[vmem, anywhere, anywhere, vmem, vmem],
        out_specs=(anywhere,) * 6,
        scratch_shapes=[
            pltpu.VMEM(memory.shape, F32),
            pltpu.VMEM((2, R, H), BF16),
            pltpu.VMEM((2, chips, wide, H), BF16),
            pltpu.VMEM((2, width, F), BF16),
            pltpu.VMEM((chips, count, wide), BF16),
            pltpu.VMEM((chips, count, wide), BF16),
            pltpu.VMEM((FB, count, wide), BF16),
            pltpu.VMEM((count, H), F32),
            pltpu.VMEM((count, H), F32),
            pltpu.VMEM((count, H), BF16),
            pltpu.VMEM((count, H), BF16),
            pltpu.VMEM((count, H), BF16),
            pltpu.VMEM((n_head, chips, count, wide), BF16),
            pltpu.VMEM((chips, count, wide), BF16),
            pltpu.VMEM((count, 1), F32),
            pltpu.VMEM((n_seq, 1, count), F32),
            pltpu.VMEM((EARLY, wide, H), BF16),
            pltpu.VMEM((EARLY, R, H), BF16),
            pltpu.VMEM((EARLY, R, H), BF16),
            dma((2, 4, chips, PIECES)),
            dma((2, n_seq, PIECES)),
            dma((n_seq,)),
            dma((n_seq,)),
            dma((2, max(n_head - 1, 1), FB)),
            dma((2, chips)),
            dma((max(n_head - 1, 1), chips)),
            dma((n_head, chips)),
            dma((3,)),
            dma((5 + EARLY,)),
            dma((2, chips)),
            dma((2, EARLY)),
            dma((2, EARLY)),
            dma,
        ],
        compiler_params=pltpu.CompilerParams(
            collective_id=0, has_side_effects=True, vmem_limit_bytes=VMEM_LIMIT
        ),
    )(tok, qkv, memory, rate_w, forget)


def backward_kernel(
    n_seq, n_head,
    xx_in, yy_in, q_in, v_in, recall_in, g_in, persist,
    grad, attended,
    xx, yy, query, values, recall, got, recalled, G, from_core, from_side, from_left, from_right, acc,
    c_send, c_recv, s_send, s_recv, z_send, l_recv, r_recv, x_send, x_recv, in_sem,
):
    me = Place(n_seq, n_head)
    L, line, side, core, head = me.length, me.line, me.side, me.core, me.head
    count, wide = xx.shape[2], xx.shape[3]
    R, H = acc.shape
    FB = query.shape[0]
    base = head * FB
    peers = me.peers()

    pairs = (
        (recall_in, recall), (xx_in.at[1], xx.at[1]), (yy_in.at[1], yy.at[1]), (xx_in.at[0], xx.at[0]),
        (yy_in.at[0], yy.at[0]), (q_in, query), (v_in, values),
        *[(g_in.at[i], from_side.at[1, me.order(i)]) for i in range(EARLY)],
    )
    loads = [pltpu.make_async_copy(a, b, in_sem.at[i]) for i, (a, b) in enumerate(pairs)]
    for c in loads:
        c.start()

    barrier = pltpu.get_barrier_semaphore()

    def greet(where):
        pl.semaphore_signal(barrier, inc=1, device_id=where, device_id_type=MESH)

    greet(me.at(line, side, 1 - core))
    greet(me.at(line, 1 - side, core))

    @pl.when(line > 0)
    def _():
        greet(me.at(line - 1, side, core))

    @pl.when(line < L - 1)
    def _():
        greet(me.at(line + 1, side, core))

    for peer in peers:
        greet(peer)
    ends = jnp.where(line > 0, 1, 0) + jnp.where(line < L - 1, 1, 0)
    pl.semaphore_wait(barrier, 2 + n_head - 1 + ends)

    def rcopy(b, p):
        there = peers[p]["head"] * FB
        return remote(recall.at[there + b], got.at[head, b], x_send.at[p, b], x_recv.at[head, b], peers[p])

    loads[0].wait()

    @pl.loop(0, FB)
    def _(b):
        for p in range(n_head - 1):
            rcopy(b, p).start()

    for c in loads[1:3]:
        c.wait()

    mine = pl.ds(pl.multiple_of(core * R, R), R)
    theirs = pl.ds(pl.multiple_of((1 - core) * R, R), R)

    def core_copy(w, j):
        return remote(
            G.at[w, j, theirs, :], from_core.at[w, j], c_send.at[w, j], c_recv.at[w, j],
            me.at(line, side, 1 - core),
        )

    def side_copy(w, l):
        return remote(
            G.at[w, l * 2 + 1 - side, mine, :], from_side.at[w, l], s_send.at[w, l], s_recv.at[w, l],
            me.at(line, 1 - side, core),
        )

    def right_copy(w, l):
        return remote(
            G.at[w, l * 2 + side, mine, :], from_left.at[w, l], z_send.at[w, l], l_recv.at[w, l],
            me.at(line + 1, side, core),
        )

    def left_copy(w, l):
        return remote(
            G.at[w, l * 2 + side, mine, :], from_right.at[w, l], z_send.at[w, l], r_recv.at[w, l],
            me.at(line - 1, side, core),
        )

    def partial(w, j):
        G[w, j] = dot_tn(xx[w, j], yy[w]).astype(BF16)
        core_copy(w, j).start()

    there = 2 * L - EARLY

    def across(n):
        w = jnp.where(n < L - EARLY, 1, 0)
        return w, me.order(L - 1 - n + (1 - w) * (L - EARLY))

    @pl.loop(0, there + 1)
    def _(n):
        @pl.when(n == L - EARLY)
        def _():
            loads[3].wait()
            loads[4].wait()

        @pl.when(n < there)
        def _():
            w, l = across(n)
            partial(w, l * 2 + 1 - side)

        @pl.when(n > 0)
        def _():
            w, l = across(n - 1)
            j = l * 2 + 1 - side
            core_copy(w, j).wait_recv()
            both = G[w, j, mine, :].astype(F32) + from_core[w, j].astype(F32)
            G[w, j, mine, :] = both.astype(BF16)
            side_copy(w, l).start()

    for c in loads[5:]:
        c.wait()

    far = L - 1

    def along(n):
        w, at = 1 - n // far, n % far
        at_end = (w == 1) & ((line == 0) | (line == L - 1))
        i = jnp.where(at_end, jnp.where(at == 0, 1, L - at), L - 1 - at)
        own = n >= 2 * far
        return jnp.where(own, 1 - (n - 2 * far), w), jnp.where(own, 0, i)

    heads_here = FB * wide // HEAD_DIM
    per = wide // HEAD_DIM
    chunk = count // 2
    scale = HEAD_DIM ** (-0.5)
    persist_count = persist.shape[1]

    def attend(n):
        b = n // per
        cols = pl.ds(pl.multiple_of((n % per) * HEAD_DIM, HEAD_DIM), HEAD_DIM)
        flat = pl.ds(pl.multiple_of(n * HEAD_DIM, HEAD_DIM), HEAD_DIM)
        for part in range(2):
            seen = (part + 1) * chunk
            q = query[b, pl.ds(part * chunk, chunk), cols]
            row = lax.broadcasted_iota(jnp.int32, (chunk, seen), 0) + part * chunk
            visible = lax.broadcasted_iota(jnp.int32, (chunk, seen), 1) <= row
            rec = recalled[b, pl.ds(0, seen), cols]
            key = xx[0, base + b, pl.ds(0, seen), cols]
            val = values[b, pl.ds(0, seen), cols]
            s0 = dot_nt(q, persist[0, :, flat]) * scale
            s1 = jnp.where(visible, dot_nt(q, rec) * scale, -1e30)
            s2 = jnp.where(visible, dot_nt(q, key) * scale, -1e30)
            top = jnp.maximum(
                jnp.max(s0, axis=1, keepdims=True),
                jnp.maximum(jnp.max(s1, axis=1, keepdims=True), jnp.max(s2, axis=1, keepdims=True)),
            )
            e0, e1, e2 = jnp.exp(s0 - top), jnp.exp(s1 - top), jnp.exp(s2 - top)
            norm = 1.0 / (
                jnp.sum(e0, axis=1, keepdims=True)
                + jnp.sum(e1, axis=1, keepdims=True)
                + jnp.sum(e2, axis=1, keepdims=True)
            )
            out = dot((e0 * norm).astype(BF16), persist[1, :, flat])
            out = out + dot((e1 * norm).astype(BF16), rec)
            out = out + dot((e2 * norm).astype(BF16), val)
            attended[pl.ds(part * chunk, chunk), flat] = out.astype(BF16)

    def recall_all():
        @pl.loop(0, FB)
        def _(b):
            total = recall[base + b].astype(F32)
            for by in range(1, n_head):
                other = (head + by) % n_head
                remote(
                    got.at[other, b], got.at[other, b], x_send.at[0, b], x_recv.at[other, b], peers[0]
                ).wait_recv()
                total = total + got[other, b].astype(F32)
            recalled[b] = total.astype(BF16)

    each = -(-heads_here // 2)

    @pl.loop(0, 2 * L)
    def _(n):
        w, i = along(n)
        l = me.order(i)
        j = l * 2 + side
        partial(w, j)

        @pl.when(n == far)
        def _():
            recall_all()

        @pl.loop(jnp.maximum((n - far) * each, 0), jnp.clip((n - far + 1) * each, 0, heads_here))
        def _(k):
            attend(k)

        core_copy(w, j).wait_recv()

        @pl.when((w == 0) | (i >= EARLY))
        def _():
            remote(
                from_side.at[w, l], from_side.at[w, l], s_send.at[w, l], s_recv.at[w, l],
                me.at(line, 1 - side, core),
            ).wait_recv()

        acc[...] = G[w, j, mine, :].astype(F32) + from_core[w, j].astype(F32) + from_side[w, l].astype(F32)

        @pl.when((l >= line) & (line > 0))
        def _():
            remote(
                from_left.at[w, l], from_left.at[w, l], z_send.at[w, l], l_recv.at[w, l],
                me.at(line - 1, side, core),
            ).wait_recv()
            acc[...] += from_left[w, l].astype(F32)

        @pl.when((l <= line) & (line < L - 1))
        def _():
            remote(
                from_right.at[w, l], from_right.at[w, l], z_send.at[w, l], r_recv.at[w, l],
                me.at(line + 1, side, core),
            ).wait_recv()
            acc[...] += from_right[w, l].astype(F32)

        @pl.when(l == line)
        def _():
            grad[w] = acc[...]

        @pl.when(l != line)
        def _():
            G[w, j, mine, :] = acc[...].astype(BF16)

        @pl.when(l > line)
        def _():
            right_copy(w, l).start()

        @pl.when(l < line)
        def _():
            left_copy(w, l).start()

    @pl.loop(0, FB)
    def _(b):
        for p in range(n_head - 1):
            rcopy(b, p).wait_send()

    @pl.loop(0, there)
    def _(n):
        w, l = across(n)
        core_copy(w, l * 2 + 1 - side).wait_send()
        side_copy(w, l).wait_send()

    @pl.loop(0, L)
    def _(l):
        for w in range(2):
            core_copy(w, l * 2 + side).wait_send()

            @pl.when(l > line)
            def _():
                right_copy(w, l).wait_send()

            @pl.when(l < line)
            def _():
                left_copy(w, l).wait_send()


def backward(xx, yy, query, values, recall, early, persist, n_seq, n_head, R):
    _, chips, count, wide = xx.shape
    H, FB = yy.shape[2], query.shape[0]
    L = n_seq // 4
    anywhere = pl.BlockSpec(memory_space=pl.ANY)
    vmem = pl.BlockSpec(memory_space=pltpu.VMEM)
    S = jax.ShapeDtypeStruct
    dma = pltpu.SemaphoreType.DMA
    return pl.pallas_call(
        functools.partial(backward_kernel, n_seq, n_head),
        out_shape=(S((2, R, H), F32), S((count, FB * wide), BF16)),
        in_specs=[anywhere] * 6 + [vmem],
        out_specs=(vmem, vmem),
        scratch_shapes=[
            pltpu.VMEM((2, chips, count, wide), BF16),
            pltpu.VMEM((2, count, H), BF16),
            pltpu.VMEM((FB, count, wide), BF16),
            pltpu.VMEM((FB, count, wide), BF16),
            pltpu.VMEM((chips, count, wide), BF16),
            pltpu.VMEM((n_head, FB, count, wide), BF16),
            pltpu.VMEM((FB, count, wide), BF16),
            pltpu.VMEM((2, chips, wide, H), BF16),
            pltpu.VMEM((2, chips, R, H), BF16),
            pltpu.VMEM((2, L, R, H), BF16),
            pltpu.VMEM((2, L, R, H), BF16),
            pltpu.VMEM((2, L, R, H), BF16),
            pltpu.VMEM((R, H), F32),
            dma((2, chips)),
            dma((2, chips)),
            dma((2, L)),
            dma((2, L)),
            dma((2, L)),
            dma((2, L)),
            dma((2, L)),
            dma((max(n_head - 1, 1), FB)),
            dma((n_head, FB)),
            dma((7 + EARLY,)),
        ],
        compiler_params=pltpu.CompilerParams(
            collective_id=1, has_side_effects=True, vmem_limit_bytes=VMEM_LIMIT
        ),
    )(xx, yy, query, values, recall, early, persist)


def interleave(x):
    R, two, H = x.shape
    return x.reshape(R, two, H // LANES, LANES).transpose(0, 2, 1, 3).reshape(R * two * H // LANES, LANES)


def layered(x, R, H):
    return x.reshape(R, H // LANES, 2, LANES).transpose(0, 2, 1, 3).reshape(R, 2, H)


def update_kernel(decay, share, grad, memory, momentum, memory_out, momentum_out):
    _, rows, H = grad.shape
    each = 2 * H // LANES
    for k in range(2):
        for tile in range(H // LANES):
            at = pl.ds(tile * 2 + k, rows, stride=each)
            new = decay[0] * momentum[at, :] - grad[k, :, tile * LANES : (tile + 1) * LANES]
            momentum_out[at, :] = new
            memory_out[at, :] = (1.0 - share[0]) * memory[at, :] + new


def update(decay, share, grad, memory, momentum):
    _, R, H = grad.shape
    step = R // 4
    each = 2 * H // LANES
    smem = pl.BlockSpec(memory_space=pltpu.SMEM)
    flat = pl.BlockSpec((step * each, LANES), lambda i: (i, 0))
    out = jax.ShapeDtypeStruct((R * each, LANES), F32)
    new_memory, new_momentum = pl.pallas_call(
        update_kernel,
        grid=(4,),
        out_shape=(out, out),
        in_specs=[smem, smem, pl.BlockSpec((2, step, H), lambda i: (0, i, 0)), flat, flat],
        out_specs=(flat, flat),
    )(decay, share, grad, interleave(memory), interleave(momentum))
    return layered(new_memory, R, H), layered(new_momentum, R, H)


def on_device(
    tokens, qkv_weight, persistent, rate_weight, forget_rate, momentum_decay, forget_share, memory, momentum
):
    n_seq, n_head = lax.axis_size("seq"), lax.axis_size("head")
    seg_len, width = tokens.shape[1], tokens.shape[2]
    lr_scale = 2.0 / (width * n_seq * seg_len) ** 0.5
    R, _, H = memory.shape
    memory_tiles = interleave(memory)
    qkv = jnp.transpose(qkv_weight, (1, 0, 2))
    xx, yy, query, values, recall, early = forward(
        tokens[0], qkv, memory_tiles, rate_weight[None], forget_rate, R, H, n_seq, n_head, lr_scale
    )
    grad, attended = backward(xx, yy, query, values, recall, early, persistent, n_seq, n_head, R)
    memory, momentum = update(momentum_decay, forget_share, grad, memory, momentum)
    return (attended[None], memory, momentum)


def solution(mesh):
    placed = (
        P(None, "seq", None),
        P(None, None, "head"),
        P(None, None, "head"),
        P(),
        P(None, "seq"),
        P(),
        P(),
        P("seq", None, "head"),
        P("seq", None, "head"),
    )
    return jax.shard_map(
        on_device,
        mesh=mesh,
        in_specs=placed,
        out_specs=(P(None, "seq", "head"), P("seq", None, "head"), P("seq", None, "head")),
        check_vma=False,
    )
```

```python
import functools

import jax
import jax.numpy as jnp
from jax import lax
from jax.experimental import pallas as pl
from jax.experimental.pallas import tpu as pltpu
from jax.sharding import PartitionSpec as P

HEAD_DIM = 128
LANES = 128
MESH = pl.DeviceIdType.MESH
VMEM_LIMIT = 67043328
PIECES = 2
EARLY = 2
UPDATE_STEPS = 2
F32, BF16 = jnp.float32, jnp.bfloat16


def remote(src, dst, send_sem, recv_sem, where):
    return pltpu.make_async_remote_copy(
        src_ref=src,
        dst_ref=dst,
        send_sem=send_sem,
        recv_sem=recv_sem,
        device_id=where,
        device_id_type=MESH,
    )


def dot(a, b):
    return jnp.dot(a, b, preferred_element_type=F32)


def dot_nt(a, b):
    return lax.dot_general(a, b, (((1,), (1,)), ((), ())), preferred_element_type=F32)


def dot_tn(a, b):
    return lax.dot_general(a, b, (((0,), (0,)), ((), ())), preferred_element_type=F32)


class Place:
    def __init__(self, n_seq, n_head):
        self.n_seq, self.n_head = n_seq, n_head
        self.length = n_seq // 4
        self.seq, self.head = lax.axis_index("seq"), lax.axis_index("head")
        self.line = self.seq // 4
        self.side = (self.seq // 2) % 2
        self.core = self.seq % 2

    def at(self, line, side, core):
        return {"seq": (line * 2 + side) * 2 + core}

    def order(self, i):
        left, right = self.line, self.length - 1 - self.line
        both = jnp.minimum(left, right)
        paired = i <= 2 * both
        step = jnp.where(paired, (i + 1) // 2, i - both)
        to_left = jnp.where(paired, i % 2 == 1, left > right)
        return jnp.where(to_left, self.line - step, self.line + step)

    def peers(self):
        return [{"head": (self.head + by) % self.n_head} for by in range(1, self.n_head)]


def rows_loop(total, step, body):
    @pl.loop(0, total // step)
    def _(i):
        body(pl.ds(pl.multiple_of(i * step, step), step))


def forward_kernel(
    n_seq, n_head, lr_scale,
    tok, qkv, memory, rate_w, forget,
    xx_out, yy_out, q_out, v_out, recall_out, g_out,
    staged, own, W, wbuf, keys, query, values, zk, zz, hk, hq, wh, errs, recall, weight, frb, G, from_core, from_side,
    w_send, w_recv, f_send, f_recv, k_send, k_recv, e_send, e_recv, qkv_sem, out_sem, block_sem, g_send, g_recv, mem_sem,
):
    me = Place(n_seq, n_head)
    L, line, side, core, head = me.length, me.line, me.side, me.core, me.head
    chips = n_seq // 2
    count, width = tok.shape
    R, H = own.shape[1:]
    wide = 2 * R
    FB = values.shape[0]
    base = head * FB
    peers = me.peers()

    memory_load = pltpu.make_async_copy(memory, staged, mem_sem)
    memory_load.start()
    loads = [pltpu.make_async_copy(qkv.at[k], wbuf.at[s], qkv_sem.at[k]) for k, s in ((1, 0), (0, 1), (2, 0))]
    loads[0].start()
    loads[1].start()

    barrier = pltpu.get_barrier_semaphore()
    for by in range(1, n_seq):
        pl.semaphore_signal(barrier, inc=1, device_id={"seq": (me.seq + by) % n_seq}, device_id_type=MESH)
    for peer in peers:
        pl.semaphore_signal(barrier, inc=1, device_id=peer, device_id_type=MESH)
    def cast(k):
        for tile in range(H // LANES):
            tiles = staged[pl.ds(tile * 2 + k, R, stride=2 * H // LANES), :]
            own[k, :, tile * LANES : (tile + 1) * LANES] = tiles.astype(BF16)

    memory_load.wait()
    cast(0)
    pl.semaphore_wait(barrier, n_seq - 1 + n_head - 1)

    piece = R // PIECES

    def block(w, l, m, c, p):
        return W.at[w, l * 2 + m, pl.ds(pl.multiple_of(c * R + p * piece, piece), piece), :]

    def copy(w, l, m, c, p, way, mine=False):
        where = (
            me.at(line + 1, side, core),
            me.at(line - 1, side, core),
            me.at(line, 1 - side, core),
            me.at(line, side, 1 - core),
        )[way]
        dst = block(w, l, m, c, p)
        src = own.at[w, pl.ds(pl.multiple_of(p * piece, piece), piece), :] if mine else dst
        chip = l * 2 + m
        return remote(src, dst, w_send.at[w, way, chip, p], w_recv.at[w, chip * 2 + c, p], where)

    def spread(w, l, p, act, ways=(0, 1, 2, 3), mine=False):
        if 0 in ways:

            @pl.when((l <= line) & (line < L - 1))
            def _():
                act(copy(w, l, side, core, p, 0, mine))

        if 1 in ways:

            @pl.when((l >= line) & (line > 0))
            def _():
                act(copy(w, l, side, core, p, 1, mine))

        for way in (2, 3):
            if way in ways:
                act(copy(w, l, side, core, p, way, mine))

    def start(c):
        c.start()

    def arrived(w, l, m, c, p):
        copy(w, l, m, c, p, 2).wait_recv()

    def start_own(w, ways):
        for p in range(PIECES):
            spread(w, line, p, start, ways, True)

    for p in range(PIECES):
        spread(0, line, p, start, (0, 1, 3), True)
    spread(0, line, 0, start, (2,), True)
    cast(1)
    fcopies = []
    for by in range(1, n_seq):
        fcopies.append(
            remote(forget, frb.at[me.seq], f_send.at[by], f_recv.at[me.seq], {"seq": (me.seq + by) % n_seq})
        )
    for c in fcopies:
        c.start()
    frb[me.seq] = forget[...]

    def xcopy(which, buf, b, p):
        return remote(
            buf.at[base + b], buf.at[base + b], k_send.at[which, p, b], k_recv.at[which, base + b], peers[p]
        )

    def project(slot, b):
        cols = pl.ds(pl.multiple_of(b * wide, wide), wide)
        return dot(tok[...], wbuf[slot, :, cols]).astype(BF16)

    def project_shared(which, buf, slot):
        loads[which].wait()

        @pl.loop(0, FB)
        def _(b):
            buf[base + b] = project(slot, b)
            for p in range(n_head - 1):
                xcopy(which, buf, b, p).start()

    def project_values():
        loads[2].wait()

        @pl.loop(0, FB)
        def _(b):
            values[b] = project(0, b)

    def weigh(rows, start_row, later):
        x = tok[rows, :].astype(F32)
        rate = jnp.sum(x * rate_w[...], axis=1, keepdims=True)
        n = x.shape[0]
        t = lax.broadcasted_iota(jnp.int32, (n, count), 0) + start_row
        u = lax.broadcasted_iota(jnp.int32, (n, count), 1)
        tail = jnp.sum(jnp.where(u > t, forget[...], 0.0), axis=1, keepdims=True) + later
        weight[rows, :] = lr_scale * jax.nn.sigmoid(rate) * jnp.exp(-tail)

    def weigh_all():
        for by in range(1, n_seq):
            other = (me.seq + by) % n_seq
            remote(forget, frb.at[other], f_send.at[by], f_recv.at[other], {"seq": other}).wait_recv()
        totals = jnp.sum(frb[...], axis=2, keepdims=True)
        which_seq = lax.broadcasted_iota(jnp.int32, totals.shape, 0)
        later = jnp.sum(jnp.where(which_seq > me.seq, totals, 0.0), axis=(0, 1, 2), keepdims=True)[0]

        @pl.loop(0, count // 32)
        def _(i):
            weigh(pl.ds(pl.multiple_of(i * 32, 32), 32), i * 32, later)

    for w in range(2):
        W[w, line * 2 + side, pl.ds(pl.multiple_of(core * R, R), R), :] = own[w]
    zk[...] = jnp.zeros_like(zk)
    right = L - 1 - line

    def keys_ready(which, buf, j):
        @pl.when((j < base) | (j >= base + FB))
        def _():
            remote(buf.at[j], buf.at[j], k_send.at[which, 0, 0], k_recv.at[which, j], peers[0]).wait_recv()

    def chip(l, mm):
        return l * 2 + jnp.where(mm == 0, side, 1 - side)

    def other_core(w, l, mm):
        for p in range(PIECES):
            arrived(w, l, jnp.where(mm == 0, side, 1 - side), 1 - core, p)

    def ecopy(j, p):
        return remote(errs.at[head, j], errs.at[head, j], e_send.at[p, j], e_recv.at[head, j], peers[p])

    def move(k):
        def come(away, step, ways):
            each = away * PIECES

            @pl.when((k > 0) & (k <= 2 * each))
            def _():
                at = k - 1
                w = jnp.where(at >= each, 1, 0)
                at = at - w * each
                l = line + step * (1 + at // PIECES)
                arrived(w, l, side, core, at % PIECES)
                spread(w, l, at % PIECES, start, ways)

            @pl.when(k == each)
            def _():
                start_own(1, ways[:1])

        come(line, -1, (0, 3))
        come(right, 1, (1, 3))

        @pl.when(k == 1)
        def _():
            start_own(1, (3,))

        total = 2 * L * PIECES

        def entry(n):
            return n // (L * PIECES), me.order(n // PIECES % L), n % PIECES

        half = L * PIECES
        first = k + jnp.where(k < half, 1, 2)
        end = jnp.minimum(k + jnp.where(k < half - 1, 2, 3), total)

        @pl.loop(first, end)
        def _(n):
            w, l, p = entry(n)

            @pl.when(l == line)
            def _():
                spread(w, l, p, start, (2,), True)

            @pl.when(l != line)
            def _():
                spread(w, l, p, start, (2,))

        @pl.when((k > 0) & (k <= total))
        def _():
            w, l, p = entry(k - 1)
            arrived(w, l, 1 - side, core, p)
            copy(w, l, 1 - side, core, p, 3).start()

    def hide(rows):
        z = zk[rows, :]
        s = jax.nn.sigmoid(z)
        hid = (z * s).astype(BF16)
        hk[rows, :] = hid
        wh[rows, :] = (weight[rows, :] * hid.astype(F32)).astype(BF16)
        zk[rows, :] = weight[rows, :] * (s * (1.0 + z * (1.0 - s)))

    def hide_query(rows):
        hq[rows, :] = jax.nn.silu(zz[rows, :]).astype(BF16)

    keys_out = pltpu.make_async_copy(keys, xx_out.at[0], out_sem.at[0])
    values_out = pltpu.make_async_copy(values, v_out, out_sem.at[1])
    query_out = pltpu.make_async_copy(query.at[pl.ds(base, FB)], q_out, out_sem.at[2])
    wh_out = pltpu.make_async_copy(wh, yy_out.at[1], out_sem.at[3])

    def err_copy(j):
        return pltpu.make_async_copy(errs.at[head, j], xx_out.at[1, j], block_sem.at[0, j])

    def recall_copy(j):
        return pltpu.make_async_copy(recall.at[j], recall_out.at[j], block_sem.at[1, j])

    def add_first(i):
        @pl.loop(0, 2)
        def _(mm):
            l = me.order(i)
            other_core(0, l, mm)
            j = chip(l, mm)
            keys_ready(0, keys, j)
            zk[...] += dot(keys[j], W[0, j])

    def make_error(i, mm):
        @pl.when((i >= 0) & (i < L))
        def _():
            l = me.order(i)
            other_core(1, l, mm)
            j = chip(l, mm)
            part = dot_nt(hk[...], W[1, j])
            mine = (j >= base) & (j < base + FB)

            @pl.when(mine)
            def _():
                errs[head, j] = (part - values[j - base].astype(F32)).astype(BF16)

            @pl.when(jnp.logical_not(mine))
            def _():
                errs[head, j] = part.astype(BF16)

            for p in range(n_head - 1):
                ecopy(j, p).start()

    def make_recall(i):
        @pl.loop(0, 2)
        def _(mm):
            j = chip(me.order(i), mm)
            recall[j] = dot_nt(hq[...], W[1, j]).astype(BF16)
            recall_copy(j).start()

    def pull_error(i, mm):
        @pl.when((i >= 0) & (i < L))
        def _():
            j = chip(me.order(i), mm)
            for by in range(1, n_head):
                other = (head + by) % n_head
                remote(
                    errs.at[other, j], errs.at[other, j], e_send.at[0, j], e_recv.at[other, j], peers[0]
                ).wait_recv()
            total = errs[0, j].astype(F32)
            for p in range(1, n_head):
                total = total + errs[p, j].astype(F32)
            for p in range(n_head - 1):
                ecopy(j, p).wait_send()
            errs[head, j] = total.astype(BF16)
            err_copy(j).start()
            zz[...] += dot(errs[head, j], W[1, j])

    mine = pl.ds(pl.multiple_of(core * R, R), R)
    theirs = pl.ds(pl.multiple_of((1 - core) * R, R), R)

    def early_core(i):
        return remote(
            G.at[i, theirs, :], from_core.at[i], g_send.at[0, i], g_recv.at[0, i], me.at(line, side, 1 - core)
        )

    def early_side(i):
        return remote(
            G.at[i, mine, :], from_side.at[i], g_send.at[1, i], g_recv.at[1, i], me.at(line, 1 - side, core)
        )

    def early_partial(i):
        G[i] = dot_tn(errs[head, chip(me.order(i), 1)], wh[...]).astype(BF16)
        early_core(i).start()

    def early_on(i):
        early_core(i).wait_recv()
        G[i, mine, :] = (G[i, mine, :].astype(F32) + from_core[i].astype(F32)).astype(BF16)
        early_side(i).start()

    def add_query(low, high):
        @pl.loop(low, high)
        def _(j):
            keys_ready(1, query, j)
            zz[...] += dot(query[j], W[0, j])

    @pl.loop(0, PIECES * (2 * L + 1) + 1)
    def _(k):
        move(k)
        slot = k // PIECES
        even = k % PIECES == 0
        last = k % PIECES == PIECES - 1

        @pl.when(k == 0)
        def _():
            project_shared(0, keys, 0)
            loads[2].start()

        @pl.when(k == 1)
        def _():
            project_shared(1, query, 1)

        @pl.when(k == PIECES)
        def _():
            project_values()

        @pl.when(k == PIECES + 1)
        def _():
            weigh_all()

        @pl.when(even & (slot > 0) & (slot <= L))
        def _():
            add_first(slot - 1)

        @pl.when(k == PIECES * L)
        def _():
            keys_out.start()
            rows_loop(count, 16, hide)
            wh_out.start()
            zz[...] = jnp.zeros_like(zz)

        @pl.when(even & (slot >= L) & (slot <= 2 * L))
        def _():
            @pl.loop(jnp.where(slot == L, -1, 0), 2)
            def _(nth):
                mm = jnp.maximum(nth, 0)
                make_error(slot - L + jnp.where(nth < 0, 0, 1 - 2 * mm), mm)

        @pl.when(k == PIECES * L + 1)
        def _():
            add_query(0, chips // 2)

        @pl.when(k == PIECES * (L + 1) + 1)
        def _():
            add_query(chips // 2, chips)
            rows_loop(count, 16, hide_query)
            zz[...] = jnp.zeros_like(zz)
            values_out.start()
            query_out.start()

        @pl.when(last & (slot > L) & (slot <= 2 * L))
        def _():
            make_recall(slot - L - 1)

        @pl.when((last & (slot > L)) | (k == PIECES * (2 * L + 1)))
        def _():
            @pl.loop(jnp.where(slot == L + 1, -1, 0), 2)
            def _(nth):
                mm = jnp.maximum(nth, 0)
                pull_error(slot - L - jnp.where(nth < 0, 1, 2 * mm), mm)

        @pl.when(even & (slot > 2 * L - 2) & (slot <= 2 * L - 2 + EARLY))
        def _():
            early_on(slot - 2 * L + 1)

        @pl.when(last & (slot > 2 * L - 3) & (slot <= 2 * L - 3 + EARLY))
        def _():
            early_partial(slot - 2 * L + 2)


    def pull(rows):
        hk[rows, :] = (zz[rows, :] * zk[rows, :]).astype(BF16)

    rows_loop(count, 16, pull)
    wdz_out = pltpu.make_async_copy(hk, yy_out.at[0], out_sem.at[4])
    wdz_out.start()
    early_out = []
    for i in range(EARLY):
        early_side(i).wait_recv()
        early_out.append(pltpu.make_async_copy(from_side.at[i], g_out.at[i], out_sem.at[5 + i]))
        early_out[i].start()

    for c in fcopies:
        c.wait_send()

    @pl.loop(0, FB)
    def _(b):
        for which, buf in enumerate((keys, query)):
            for p in range(n_head - 1):
                xcopy(which, buf, b, p).wait_send()

    @pl.loop(0, L)
    def _(l):
        for w in range(2):
            for p in range(PIECES):
                spread(w, l, p, lambda c: c.wait_send())
                copy(w, l, 1 - side, core, p, 3).wait_send()

    for i in range(EARLY):
        early_core(i).wait_send()
        early_side(i).wait_send()

    @pl.loop(0, chips)
    def _(j):
        err_copy(j).wait()
        recall_copy(j).wait()

    for c in (keys_out, values_out, query_out, wh_out, wdz_out, *early_out):
        c.wait()


def forward(tok, qkv, memory, rate_w, forget, R, H, n_seq, n_head, lr_scale):
    count, width = tok.shape
    F = qkv.shape[2]
    chips, wide = n_seq // 2, 2 * R
    FB = F // wide
    assert n_seq % 4 == 0 and n_seq >= 16 and FB * wide == F and chips * wide == width
    anywhere = pl.BlockSpec(memory_space=pl.ANY)
    vmem = pl.BlockSpec(memory_space=pltpu.VMEM)
    S = jax.ShapeDtypeStruct
    dma = pltpu.SemaphoreType.DMA
    return pl.pallas_call(
        functools.partial(forward_kernel, n_seq, n_head, lr_scale),
        out_shape=(
            S((2, chips, count, wide), BF16),
            S((2, count, H), BF16),
            S((FB, count, wide), BF16),
            S((FB, count, wide), BF16),
            S((chips, count, wide), BF16),
            S((EARLY, R, H), BF16),
        ),
        in_specs=[vmem, anywhere, anywhere, vmem, vmem],
        out_specs=(anywhere,) * 6,
        scratch_shapes=[
            pltpu.VMEM(memory.shape, F32),
            pltpu.VMEM((2, R, H), BF16),
            pltpu.VMEM((2, chips, wide, H), BF16),
            pltpu.VMEM((2, width, F), BF16),
            pltpu.VMEM((chips, count, wide), BF16),
            pltpu.VMEM((chips, count, wide), BF16),
            pltpu.VMEM((FB, count, wide), BF16),
            pltpu.VMEM((count, H), F32),
            pltpu.VMEM((count, H), F32),
            pltpu.VMEM((count, H), BF16),
            pltpu.VMEM((count, H), BF16),
            pltpu.VMEM((count, H), BF16),
            pltpu.VMEM((n_head, chips, count, wide), BF16),
            pltpu.VMEM((chips, count, wide), BF16),
            pltpu.VMEM((count, 1), F32),
            pltpu.VMEM((n_seq, 1, count), F32),
            pltpu.VMEM((EARLY, wide, H), BF16),
            pltpu.VMEM((EARLY, R, H), BF16),
            pltpu.VMEM((EARLY, R, H), BF16),
            dma((2, 4, chips, PIECES)),
            dma((2, n_seq, PIECES)),
            dma((n_seq,)),
            dma((n_seq,)),
            dma((2, max(n_head - 1, 1), FB)),
            dma((2, chips)),
            dma((max(n_head - 1, 1), chips)),
            dma((n_head, chips)),
            dma((3,)),
            dma((5 + EARLY,)),
            dma((2, chips)),
            dma((2, EARLY)),
            dma((2, EARLY)),
            dma,
        ],
        compiler_params=pltpu.CompilerParams(
            collective_id=0, has_side_effects=True, vmem_limit_bytes=VMEM_LIMIT
        ),
    )(tok, qkv, memory, rate_w, forget)


def backward_kernel(
    n_seq, n_head,
    xx_in, yy_in, q_in, v_in, recall_in, g_in, persist,
    grad, attended,
    xx, yy, query, values, recall, got, recalled, G, from_core, from_side, from_left, from_right, acc,
    c_send, c_recv, s_send, s_recv, z_send, l_recv, r_recv, x_send, x_recv, in_sem,
):
    me = Place(n_seq, n_head)
    L, line, side, core, head = me.length, me.line, me.side, me.core, me.head
    count, wide = xx.shape[2], xx.shape[3]
    R, H = acc.shape
    FB = query.shape[0]
    base = head * FB
    peers = me.peers()

    pairs = (
        (recall_in, recall), (xx_in.at[1], xx.at[1]), (yy_in.at[1], yy.at[1]), (xx_in.at[0], xx.at[0]),
        (yy_in.at[0], yy.at[0]), (q_in, query), (v_in, values),
        *[(g_in.at[i], from_side.at[1, me.order(i)]) for i in range(EARLY)],
    )
    loads = [pltpu.make_async_copy(a, b, in_sem.at[i]) for i, (a, b) in enumerate(pairs)]
    for c in (loads[1], loads[2], loads[0], *loads[3:]):
        c.start()

    barrier = pltpu.get_barrier_semaphore()

    def greet(where):
        pl.semaphore_signal(barrier, inc=1, device_id=where, device_id_type=MESH)

    greet(me.at(line, side, 1 - core))
    greet(me.at(line, 1 - side, core))

    @pl.when(line > 0)
    def _():
        greet(me.at(line - 1, side, core))

    @pl.when(line < L - 1)
    def _():
        greet(me.at(line + 1, side, core))

    for peer in peers:
        greet(peer)
    ends = jnp.where(line > 0, 1, 0) + jnp.where(line < L - 1, 1, 0)
    pl.semaphore_wait(barrier, 2 + n_head - 1 + ends)

    def rcopy(b, p):
        there = peers[p]["head"] * FB
        return remote(recall.at[there + b], got.at[head, b], x_send.at[p, b], x_recv.at[head, b], peers[p])

    loads[0].wait()

    @pl.loop(0, FB)
    def _(b):
        for p in range(n_head - 1):
            rcopy(b, p).start()

    for c in loads[1:3]:
        c.wait()

    mine = pl.ds(pl.multiple_of(core * R, R), R)
    theirs = pl.ds(pl.multiple_of((1 - core) * R, R), R)

    def core_copy(w, j):
        return remote(
            G.at[w, j, theirs, :], from_core.at[w, j], c_send.at[w, j], c_recv.at[w, j],
            me.at(line, side, 1 - core),
        )

    def side_copy(w, l):
        return remote(
            G.at[w, l * 2 + 1 - side, mine, :], from_side.at[w, l], s_send.at[w, l], s_recv.at[w, l],
            me.at(line, 1 - side, core),
        )

    def right_copy(w, l):
        return remote(
            G.at[w, l * 2 + side, mine, :], from_left.at[w, l], z_send.at[w, l], l_recv.at[w, l],
            me.at(line + 1, side, core),
        )

    def left_copy(w, l):
        return remote(
            G.at[w, l * 2 + side, mine, :], from_right.at[w, l], z_send.at[w, l], r_recv.at[w, l],
            me.at(line - 1, side, core),
        )

    def partial(w, j):
        G[w, j] = dot_tn(xx[w, j], yy[w]).astype(BF16)
        core_copy(w, j).start()

    there = 2 * L - EARLY
    far = L - 1
    at_end = (line == 0) | (line == L - 1)
    low = jnp.logical_not(at_end) & (line < L // 2)

    def across(n):
        both = 2 * (L - EARLY)
        n = jnp.where(low & (n == both - 1), both, jnp.where(low & (n == both), both - 1, n))
        w = jnp.where(n < both, 1 - n % 2, 0)
        return w, me.order(jnp.where(n < both, L - 1 - n // 2, EARLY - 1 - (n - both)))

    def along(n):
        t = n - (2 * far - 4)
        last_low = 2 * far - 4 + jnp.where(t % 2 == 0, 2 + t // 2, t // 2)
        last_high = 2 * far - 4 + (t % 2) * 2 + t // 2
        inner = jnp.where(t < 0, n, jnp.where(low, last_low, last_high))
        outer = jnp.where(n == 0, 2 * far - 2, jnp.where(n == 2 * far - 1, n, n - 1))
        q = jnp.where(at_end, outer, inner)
        own = n >= 2 * far
        return jnp.where(own, 1 - (n - 2 * far), 1 - q % 2), jnp.where(own, 0, L - 1 - q // 2)

    def line_partial(n):
        w, i = along(n)
        partial(w, me.order(i) * 2 + side)

    def line_finish(n):
        w, i = along(n)
        l = me.order(i)
        j = l * 2 + side
        core_copy(w, j).wait_recv()

        @pl.when((w == 0) | (i >= EARLY))
        def _():
            remote(
                from_side.at[w, l], from_side.at[w, l], s_send.at[w, l], s_recv.at[w, l],
                me.at(line, 1 - side, core),
            ).wait_recv()

        acc[...] = G[w, j, mine, :].astype(F32) + from_core[w, j].astype(F32) + from_side[w, l].astype(F32)

        @pl.when((l >= line) & (line > 0))
        def _():
            remote(
                from_left.at[w, l], from_left.at[w, l], z_send.at[w, l], l_recv.at[w, l],
                me.at(line - 1, side, core),
            ).wait_recv()
            acc[...] += from_left[w, l].astype(F32)

        @pl.when((l <= line) & (line < L - 1))
        def _():
            remote(
                from_right.at[w, l], from_right.at[w, l], z_send.at[w, l], r_recv.at[w, l],
                me.at(line + 1, side, core),
            ).wait_recv()
            acc[...] += from_right[w, l].astype(F32)

        @pl.when(l == line)
        def _():
            for tile in range(H // LANES):
                rows = pl.ds(tile * 2 + w, R, stride=2 * H // LANES)
                grad[rows, :] = acc[:, tile * LANES : (tile + 1) * LANES]

        @pl.when(l != line)
        def _():
            G[w, j, mine, :] = acc[...].astype(BF16)

        @pl.when(l > line)
        def _():
            right_copy(w, l).start()

        @pl.when(l < line)
        def _():
            left_copy(w, l).start()

    @pl.when(at_end)
    def _():
        line_partial(0)

    @pl.loop(0, there + 1)
    def _(n):
        @pl.when(n == 1)
        def _():
            loads[3].wait()
            loads[4].wait()

        @pl.when(n < there)
        def _():
            w, l = across(n)
            partial(w, l * 2 + 1 - side)

        @pl.when(n > 0)
        def _():
            w, l = across(n - 1)
            j = l * 2 + 1 - side
            core_copy(w, j).wait_recv()
            both = G[w, j, mine, :].astype(F32) + from_core[w, j].astype(F32)
            G[w, j, mine, :] = both.astype(BF16)
            side_copy(w, l).start()

        @pl.when(n == 2)
        def _():
            for c in loads[7:]:
                c.wait()

        @pl.when((n == 2) & at_end)
        def _():
            line_finish(0)

    loads[5].wait()
    loads[6].wait()

    heads_here = FB * wide // HEAD_DIM
    per = wide // HEAD_DIM
    chunk = count // 2
    scale = HEAD_DIM ** (-0.5)
    persist_count = persist.shape[1]

    def attend(n):
        b = n // per
        cols = pl.ds(pl.multiple_of((n % per) * HEAD_DIM, HEAD_DIM), HEAD_DIM)
        flat = pl.ds(pl.multiple_of(n * HEAD_DIM, HEAD_DIM), HEAD_DIM)
        for part in range(2):
            seen = (part + 1) * chunk
            q = query[b, pl.ds(part * chunk, chunk), cols]
            row = lax.broadcasted_iota(jnp.int32, (chunk, seen), 0) + part * chunk
            visible = lax.broadcasted_iota(jnp.int32, (chunk, seen), 1) <= row
            rec = recalled[b, pl.ds(0, seen), cols]
            key = xx[0, base + b, pl.ds(0, seen), cols]
            val = values[b, pl.ds(0, seen), cols]
            s0 = dot_nt(q, persist[0, :, flat]) * scale
            s1 = jnp.where(visible, dot_nt(q, rec) * scale, -1e30)
            s2 = jnp.where(visible, dot_nt(q, key) * scale, -1e30)
            top = jnp.maximum(
                jnp.max(s0, axis=1, keepdims=True),
                jnp.maximum(jnp.max(s1, axis=1, keepdims=True), jnp.max(s2, axis=1, keepdims=True)),
            )
            e0, e1, e2 = jnp.exp(s0 - top), jnp.exp(s1 - top), jnp.exp(s2 - top)
            norm = 1.0 / (
                jnp.sum(e0, axis=1, keepdims=True)
                + jnp.sum(e1, axis=1, keepdims=True)
                + jnp.sum(e2, axis=1, keepdims=True)
            )
            out = dot((e0 * norm).astype(BF16), persist[1, :, flat])
            out = out + dot((e1 * norm).astype(BF16), rec)
            out = out + dot((e2 * norm).astype(BF16), val)
            attended[pl.ds(part * chunk, chunk), flat] = out.astype(BF16)

    def recall_all():
        @pl.loop(0, FB)
        def _(b):
            total = recall[base + b].astype(F32)
            for by in range(1, n_head):
                other = (head + by) % n_head
                remote(
                    got.at[other, b], got.at[other, b], x_send.at[0, b], x_recv.at[other, b], peers[0]
                ).wait_recv()
                total = total + got[other, b].astype(F32)
            recalled[b] = total.astype(BF16)

    each = -(-heads_here // 2)

    @pl.loop(jnp.where(at_end, 1, 0), 2 * L)
    def _(n):
        line_partial(n)

        @pl.when(n == far)
        def _():
            recall_all()

        @pl.loop(jnp.maximum((n - far) * each, 0), jnp.clip((n - far + 1) * each, 0, heads_here))
        def _(k):
            attend(k)

        line_finish(n)

    @pl.loop(0, FB)
    def _(b):
        for p in range(n_head - 1):
            rcopy(b, p).wait_send()

    @pl.loop(0, there)
    def _(n):
        w, l = across(n)
        core_copy(w, l * 2 + 1 - side).wait_send()
        side_copy(w, l).wait_send()

    @pl.loop(0, L)
    def _(l):
        for w in range(2):
            core_copy(w, l * 2 + side).wait_send()

            @pl.when(l > line)
            def _():
                right_copy(w, l).wait_send()

            @pl.when(l < line)
            def _():
                left_copy(w, l).wait_send()


def backward(xx, yy, query, values, recall, early, persist, n_seq, n_head, R):
    _, chips, count, wide = xx.shape
    H, FB = yy.shape[2], query.shape[0]
    L = n_seq // 4
    anywhere = pl.BlockSpec(memory_space=pl.ANY)
    vmem = pl.BlockSpec(memory_space=pltpu.VMEM)
    S = jax.ShapeDtypeStruct
    dma = pltpu.SemaphoreType.DMA
    return pl.pallas_call(
        functools.partial(backward_kernel, n_seq, n_head),
        out_shape=(S((R * 2 * H // LANES, LANES), F32), S((count, FB * wide), BF16)),
        in_specs=[anywhere] * 6 + [vmem],
        out_specs=(vmem, vmem),
        scratch_shapes=[
            pltpu.VMEM((2, chips, count, wide), BF16),
            pltpu.VMEM((2, count, H), BF16),
            pltpu.VMEM((FB, count, wide), BF16),
            pltpu.VMEM((FB, count, wide), BF16),
            pltpu.VMEM((chips, count, wide), BF16),
            pltpu.VMEM((n_head, FB, count, wide), BF16),
            pltpu.VMEM((FB, count, wide), BF16),
            pltpu.VMEM((2, chips, wide, H), BF16),
            pltpu.VMEM((2, chips, R, H), BF16),
            pltpu.VMEM((2, L, R, H), BF16),
            pltpu.VMEM((2, L, R, H), BF16),
            pltpu.VMEM((2, L, R, H), BF16),
            pltpu.VMEM((R, H), F32),
            dma((2, chips)),
            dma((2, chips)),
            dma((2, L)),
            dma((2, L)),
            dma((2, L)),
            dma((2, L)),
            dma((2, L)),
            dma((max(n_head - 1, 1), FB)),
            dma((n_head, FB)),
            dma((7 + EARLY,)),
        ],
        compiler_params=pltpu.CompilerParams(
            collective_id=1, has_side_effects=True, vmem_limit_bytes=VMEM_LIMIT
        ),
    )(xx, yy, query, values, recall, early, persist)


def interleave(x):
    R, two, H = x.shape
    return x.reshape(R, two, H // LANES, LANES).transpose(0, 2, 1, 3).reshape(R * two * H // LANES, LANES)


def layered(x, R, H):
    return x.reshape(R, H // LANES, 2, LANES).transpose(0, 2, 1, 3).reshape(R, 2, H)


def update_kernel(decay, share, grad, memory, momentum, memory_out, momentum_out):
    new = decay[0] * momentum[...] - grad[...]
    momentum_out[...] = new
    memory_out[...] = (1.0 - share[0]) * memory[...] + new


def update(decay, share, grad, memory, momentum):
    rows = grad.shape[0]
    smem = pl.BlockSpec(memory_space=pltpu.SMEM)
    flat = pl.BlockSpec((rows // UPDATE_STEPS, LANES), lambda i: (i, 0))
    out = jax.ShapeDtypeStruct(grad.shape, F32)
    return pl.pallas_call(
        update_kernel,
        grid=(UPDATE_STEPS,),
        out_shape=(out, out),
        in_specs=[smem, smem, flat, flat, flat],
        out_specs=(flat, flat),
    )(decay, share, grad, memory, momentum)


def on_device(
    tokens, qkv_weight, persistent, rate_weight, forget_rate, momentum_decay, forget_share, memory, momentum
):
    n_seq, n_head = lax.axis_size("seq"), lax.axis_size("head")
    seg_len, width = tokens.shape[1], tokens.shape[2]
    lr_scale = 2.0 / (width * n_seq * seg_len) ** 0.5
    R, _, H = memory.shape
    memory_tiles = interleave(memory)
    qkv = jnp.transpose(qkv_weight, (1, 0, 2))
    xx, yy, query, values, recall, early = forward(
        tokens[0], qkv, memory_tiles, rate_weight[None], forget_rate, R, H, n_seq, n_head, lr_scale
    )
    grad, attended = backward(xx, yy, query, values, recall, early, persistent, n_seq, n_head, R)
    memory, momentum = update(momentum_decay, forget_share, grad, memory_tiles, interleave(momentum))
    memory, momentum = layered(memory, R, H), layered(momentum, R, H)
    return (attended[None], memory, momentum)


def solution(mesh):
    placed = (
        P(None, "seq", None),
        P(None, None, "head"),
        P(None, None, "head"),
        P(),
        P(None, "seq"),
        P(),
        P(),
        P("seq", None, "head"),
        P("seq", None, "head"),
    )
    return jax.shard_map(
        on_device,
        mesh=mesh,
        in_specs=placed,
        out_specs=(P(None, "seq", "head"), P("seq", None, "head"), P("seq", None, "head")),
        check_vma=False,
    )
```

```python
import functools

import jax
import jax.numpy as jnp
from jax import lax
from jax.experimental import pallas as pl
from jax.experimental.pallas import tpu as pltpu
from jax.sharding import PartitionSpec as P

HEAD_DIM = 128
LANES = 128
MESH = pl.DeviceIdType.MESH
VMEM_LIMIT = 67043328
PIECES = 2
EARLY = 2
UPDATE_STEPS = 2
F32, BF16 = jnp.float32, jnp.bfloat16


def remote(src, dst, send_sem, recv_sem, where):
    return pltpu.make_async_remote_copy(
        src_ref=src,
        dst_ref=dst,
        send_sem=send_sem,
        recv_sem=recv_sem,
        device_id=where,
        device_id_type=MESH,
    )


def dot(a, b):
    return jnp.dot(a, b, preferred_element_type=F32)


def dot_nt(a, b):
    return lax.dot_general(a, b, (((1,), (1,)), ((), ())), preferred_element_type=F32)


def dot_tn(a, b):
    return lax.dot_general(a, b, (((0,), (0,)), ((), ())), preferred_element_type=F32)


class Place:
    def __init__(self, n_seq, n_head):
        self.n_seq, self.n_head = n_seq, n_head
        self.length = n_seq // 4
        self.seq, self.head = lax.axis_index("seq"), lax.axis_index("head")
        self.line = self.seq // 4
        self.side = (self.seq // 2) % 2
        self.core = self.seq % 2

    def at(self, line, side, core):
        return {"seq": (line * 2 + side) * 2 + core}

    def order(self, i):
        left, right = self.line, self.length - 1 - self.line
        both = jnp.minimum(left, right)
        paired = i <= 2 * both
        step = jnp.where(paired, (i + 1) // 2, i - both)
        to_left = jnp.where(paired, i % 2 == 1, left > right)
        return jnp.where(to_left, self.line - step, self.line + step)

    def peers(self):
        return [{"head": (self.head + by) % self.n_head} for by in range(1, self.n_head)]


def rows_loop(total, step, body):
    @pl.loop(0, total // step)
    def _(i):
        body(pl.ds(pl.multiple_of(i * step, step), step))


def forward_kernel(
    n_seq, n_head, lr_scale,
    tok_in, qkv, memory, rate_w, forget,
    xx_out, yy_out, q_out, v_out, recall_out, g_out,
    tok, staged, own, W, wbuf, keys, query, values, zk, zz, hk, hq, wh, errs, recall, weight, frb, G, from_core, from_side,
    w_send, w_recv, f_send, f_recv, k_send, k_recv, e_send, e_recv, qkv_sem, out_sem, block_sem, g_send, g_recv, mem_sem, tok_sem,
):
    me = Place(n_seq, n_head)
    L, line, side, core, head = me.length, me.line, me.side, me.core, me.head
    chips = n_seq // 2
    count, width = tok.shape
    R, H = own.shape[1:]
    wide = 2 * R
    FB = values.shape[0]
    base = head * FB
    peers = me.peers()

    memory_load = pltpu.make_async_copy(memory, staged, mem_sem)
    memory_load.start()
    tok_load = pltpu.make_async_copy(tok_in, tok, tok_sem)
    loads = [pltpu.make_async_copy(qkv.at[k], wbuf.at[s], qkv_sem.at[k]) for k, s in ((1, 0), (0, 1), (2, 0))]
    tok_load.start()
    loads[0].start()
    loads[1].start()

    barrier = pltpu.get_barrier_semaphore()
    for by in range(1, n_seq):
        pl.semaphore_signal(barrier, inc=1, device_id={"seq": (me.seq + by) % n_seq}, device_id_type=MESH)
    for peer in peers:
        pl.semaphore_signal(barrier, inc=1, device_id=peer, device_id_type=MESH)
    def cast(k):
        for tile in range(H // LANES):
            tiles = staged[pl.ds(tile * 2 + k, R, stride=2 * H // LANES), :]
            own[k, :, tile * LANES : (tile + 1) * LANES] = tiles.astype(BF16)

    memory_load.wait()
    cast(0)
    pl.semaphore_wait(barrier, n_seq - 1 + n_head - 1)

    piece = R // PIECES

    def block(w, l, m, c, p):
        return W.at[w, l * 2 + m, pl.ds(pl.multiple_of(c * R + p * piece, piece), piece), :]

    def copy(w, l, m, c, p, way, mine=False):
        where = (
            me.at(line + 1, side, core),
            me.at(line - 1, side, core),
            me.at(line, 1 - side, core),
            me.at(line, side, 1 - core),
        )[way]
        dst = block(w, l, m, c, p)
        src = own.at[w, pl.ds(pl.multiple_of(p * piece, piece), piece), :] if mine else dst
        chip = l * 2 + m
        return remote(src, dst, w_send.at[w, way, chip, p], w_recv.at[w, chip * 2 + c, p], where)

    def spread(w, l, p, act, ways=(0, 1, 2, 3), mine=False):
        if 0 in ways:

            @pl.when((l <= line) & (line < L - 1))
            def _():
                act(copy(w, l, side, core, p, 0, mine))

        if 1 in ways:

            @pl.when((l >= line) & (line > 0))
            def _():
                act(copy(w, l, side, core, p, 1, mine))

        for way in (2, 3):
            if way in ways:
                act(copy(w, l, side, core, p, way, mine))

    def start(c):
        c.start()

    def arrived(w, l, m, c, p):
        copy(w, l, m, c, p, 2).wait_recv()

    def start_own(w, ways):
        for p in range(PIECES):
            spread(w, line, p, start, ways, True)

    for p in range(PIECES):
        spread(0, line, p, start, (0, 1, 3), True)
    spread(0, line, 0, start, (2,), True)
    cast(1)
    fcopies = []
    for by in range(1, n_seq):
        fcopies.append(
            remote(forget, frb.at[me.seq], f_send.at[by], f_recv.at[me.seq], {"seq": (me.seq + by) % n_seq})
        )
    for c in fcopies:
        c.start()
    frb[me.seq] = forget[...]

    def xcopy(which, buf, b, p):
        return remote(
            buf.at[base + b], buf.at[base + b], k_send.at[which, p, b], k_recv.at[which, base + b], peers[p]
        )

    def project(slot, b):
        cols = pl.ds(pl.multiple_of(b * wide, wide), wide)
        return dot(tok[...], wbuf[slot, :, cols]).astype(BF16)

    def project_shared(which, buf, slot):
        loads[which].wait()

        @pl.loop(0, FB)
        def _(b):
            buf[base + b] = project(slot, b)
            for p in range(n_head - 1):
                xcopy(which, buf, b, p).start()

    def project_values():
        loads[2].wait()

        @pl.loop(0, FB)
        def _(b):
            values[b] = project(0, b)

    def weigh(rows, start_row, later):
        x = tok[rows, :].astype(F32)
        rate = jnp.sum(x * rate_w[...], axis=1, keepdims=True)
        n = x.shape[0]
        t = lax.broadcasted_iota(jnp.int32, (n, count), 0) + start_row
        u = lax.broadcasted_iota(jnp.int32, (n, count), 1)
        tail = jnp.sum(jnp.where(u > t, forget[...], 0.0), axis=1, keepdims=True) + later
        weight[rows, :] = lr_scale * jax.nn.sigmoid(rate) * jnp.exp(-tail)

    def weigh_all():
        for by in range(1, n_seq):
            other = (me.seq + by) % n_seq
            remote(forget, frb.at[other], f_send.at[by], f_recv.at[other], {"seq": other}).wait_recv()
        totals = jnp.sum(frb[...], axis=2, keepdims=True)
        which_seq = lax.broadcasted_iota(jnp.int32, totals.shape, 0)
        later = jnp.sum(jnp.where(which_seq > me.seq, totals, 0.0), axis=(0, 1, 2), keepdims=True)[0]

        @pl.loop(0, count // 32)
        def _(i):
            weigh(pl.ds(pl.multiple_of(i * 32, 32), 32), i * 32, later)

    for w in range(2):
        W[w, line * 2 + side, pl.ds(pl.multiple_of(core * R, R), R), :] = own[w]
    zk[...] = jnp.zeros_like(zk)
    right = L - 1 - line

    def keys_ready(which, buf, j):
        @pl.when((j < base) | (j >= base + FB))
        def _():
            remote(buf.at[j], buf.at[j], k_send.at[which, 0, 0], k_recv.at[which, j], peers[0]).wait_recv()

    def chip(l, mm):
        return l * 2 + jnp.where(mm == 0, side, 1 - side)

    def other_core(w, l, mm):
        for p in range(PIECES):
            arrived(w, l, jnp.where(mm == 0, side, 1 - side), 1 - core, p)

    def ecopy(j, p):
        return remote(errs.at[head, j], errs.at[head, j], e_send.at[p, j], e_recv.at[head, j], peers[p])

    def move(k):
        def come(away, step, ways):
            each = away * PIECES

            @pl.when((k > 0) & (k <= 2 * each))
            def _():
                at = k - 1
                w = jnp.where(at >= each, 1, 0)
                at = at - w * each
                l = line + step * (1 + at // PIECES)
                arrived(w, l, side, core, at % PIECES)
                spread(w, l, at % PIECES, start, ways)

            @pl.when(k == each)
            def _():
                start_own(1, ways[:1])

        come(line, -1, (0, 3))
        come(right, 1, (1, 3))

        @pl.when(k == 1)
        def _():
            start_own(1, (3,))

        total = 2 * L * PIECES

        def entry(n):
            return n // (L * PIECES), me.order(n // PIECES % L), n % PIECES

        half = L * PIECES
        first = k + jnp.where(k < half, 1, 2)
        end = jnp.minimum(k + jnp.where(k < half - 1, 2, 3), total)

        @pl.loop(first, end)
        def _(n):
            w, l, p = entry(n)

            @pl.when(l == line)
            def _():
                spread(w, l, p, start, (2,), True)

            @pl.when(l != line)
            def _():
                spread(w, l, p, start, (2,))

        @pl.when((k > 0) & (k <= total))
        def _():
            w, l, p = entry(k - 1)
            arrived(w, l, 1 - side, core, p)
            copy(w, l, 1 - side, core, p, 3).start()

    def hide(rows):
        z = zk[rows, :]
        s = jax.nn.sigmoid(z)
        hid = (z * s).astype(BF16)
        hk[rows, :] = hid
        wh[rows, :] = (weight[rows, :] * hid.astype(F32)).astype(BF16)
        zk[rows, :] = weight[rows, :] * (s * (1.0 + z * (1.0 - s)))

    def hide_query(rows):
        hq[rows, :] = jax.nn.silu(zz[rows, :]).astype(BF16)

    keys_out = pltpu.make_async_copy(keys, xx_out.at[0], out_sem.at[0])
    values_out = pltpu.make_async_copy(values, v_out, out_sem.at[1])
    query_out = pltpu.make_async_copy(query.at[pl.ds(base, FB)], q_out, out_sem.at[2])
    wh_out = pltpu.make_async_copy(wh, yy_out.at[1], out_sem.at[3])

    def err_copy(j):
        return pltpu.make_async_copy(errs.at[head, j], xx_out.at[1, j], block_sem.at[0, j])

    def recall_copy(j):
        return pltpu.make_async_copy(recall.at[j], recall_out.at[j], block_sem.at[1, j])

    def add_first(i):
        @pl.loop(0, 2)
        def _(mm):
            l = me.order(i)
            other_core(0, l, mm)
            j = chip(l, mm)
            keys_ready(0, keys, j)
            zk[...] += dot(keys[j], W[0, j])

    def make_error(i, mm):
        @pl.when((i >= 0) & (i < L))
        def _():
            l = me.order(i)
            other_core(1, l, mm)
            j = chip(l, mm)
            part = dot_nt(hk[...], W[1, j])
            mine = (j >= base) & (j < base + FB)

            @pl.when(mine)
            def _():
                errs[head, j] = (part - values[j - base].astype(F32)).astype(BF16)

            @pl.when(jnp.logical_not(mine))
            def _():
                errs[head, j] = part.astype(BF16)

            for p in range(n_head - 1):
                ecopy(j, p).start()

    def make_recall(i):
        @pl.loop(0, 2)
        def _(mm):
            j = chip(me.order(i), mm)
            recall[j] = dot_nt(hq[...], W[1, j]).astype(BF16)
            recall_copy(j).start()

    def pull_error(i, mm):
        @pl.when((i >= 0) & (i < L))
        def _():
            j = chip(me.order(i), mm)
            for by in range(1, n_head):
                other = (head + by) % n_head
                remote(
                    errs.at[other, j], errs.at[other, j], e_send.at[0, j], e_recv.at[other, j], peers[0]
                ).wait_recv()
            total = errs[0, j].astype(F32)
            for p in range(1, n_head):
                total = total + errs[p, j].astype(F32)
            for p in range(n_head - 1):
                ecopy(j, p).wait_send()
            errs[head, j] = total.astype(BF16)
            err_copy(j).start()
            zz[...] += dot(errs[head, j], W[1, j])

    mine = pl.ds(pl.multiple_of(core * R, R), R)
    theirs = pl.ds(pl.multiple_of((1 - core) * R, R), R)

    def early_core(i):
        return remote(
            G.at[i, theirs, :], from_core.at[i], g_send.at[0, i], g_recv.at[0, i], me.at(line, side, 1 - core)
        )

    def early_side(i):
        return remote(
            G.at[i, mine, :], from_side.at[i], g_send.at[1, i], g_recv.at[1, i], me.at(line, 1 - side, core)
        )

    def early_partial(i):
        G[i] = dot_tn(errs[head, chip(me.order(i), 1)], wh[...]).astype(BF16)
        early_core(i).start()

    def early_on(i):
        early_core(i).wait_recv()
        G[i, mine, :] = (G[i, mine, :].astype(F32) + from_core[i].astype(F32)).astype(BF16)
        early_side(i).start()

    def add_query(low, high):
        @pl.loop(low, high)
        def _(j):
            keys_ready(1, query, j)
            zz[...] += dot(query[j], W[0, j])

    @pl.loop(0, PIECES * (2 * L + 1) + 1)
    def _(k):
        move(k)
        slot = k // PIECES
        even = k % PIECES == 0
        last = k % PIECES == PIECES - 1

        @pl.when(k == 0)
        def _():
            tok_load.wait()
            project_shared(0, keys, 0)
            loads[2].start()

        @pl.when(k == 1)
        def _():
            project_shared(1, query, 1)

        @pl.when(k == PIECES)
        def _():
            project_values()

        @pl.when(k == PIECES + 1)
        def _():
            weigh_all()

        @pl.when(even & (slot > 0) & (slot <= L))
        def _():
            add_first(slot - 1)

        @pl.when(k == PIECES * L)
        def _():
            keys_out.start()
            rows_loop(count, 16, hide)
            wh_out.start()
            zz[...] = jnp.zeros_like(zz)

        @pl.when(even & (slot >= L) & (slot <= 2 * L))
        def _():
            @pl.loop(jnp.where(slot == L, -1, 0), 2)
            def _(nth):
                mm = jnp.maximum(nth, 0)
                make_error(slot - L + jnp.where(nth < 0, 0, 1 - 2 * mm), mm)

        @pl.when(k == PIECES * L + 1)
        def _():
            add_query(0, chips // 2)

        @pl.when(k == PIECES * (L + 1) + 1)
        def _():
            add_query(chips // 2, chips)
            rows_loop(count, 16, hide_query)
            zz[...] = jnp.zeros_like(zz)
            values_out.start()
            query_out.start()

        @pl.when(last & (slot > L) & (slot <= 2 * L))
        def _():
            make_recall(slot - L - 1)

        @pl.when((last & (slot > L)) | (k == PIECES * (2 * L + 1)))
        def _():
            @pl.loop(jnp.where(slot == L + 1, -1, 0), 2)
            def _(nth):
                mm = jnp.maximum(nth, 0)
                pull_error(slot - L - jnp.where(nth < 0, 1, 2 * mm), mm)

        @pl.when(even & (slot > 2 * L - 2) & (slot <= 2 * L - 2 + EARLY))
        def _():
            early_on(slot - 2 * L + 1)

        @pl.when(last & (slot > 2 * L - 3) & (slot <= 2 * L - 3 + EARLY))
        def _():
            early_partial(slot - 2 * L + 2)


    def pull(rows):
        hk[rows, :] = (zz[rows, :] * zk[rows, :]).astype(BF16)

    rows_loop(count, 16, pull)
    wdz_out = pltpu.make_async_copy(hk, yy_out.at[0], out_sem.at[4])
    wdz_out.start()

    for c in fcopies:
        c.wait_send()

    @pl.loop(0, FB)
    def _(b):
        for which, buf in enumerate((keys, query)):
            for p in range(n_head - 1):
                xcopy(which, buf, b, p).wait_send()

    @pl.loop(0, L)
    def _(l):
        for w in range(2):
            for p in range(PIECES):
                spread(w, l, p, lambda c: c.wait_send())
                copy(w, l, 1 - side, core, p, 3).wait_send()

    @pl.loop(0, chips)
    def _(j):
        err_copy(j).wait()
        recall_copy(j).wait()

    early_out = []
    for i in range(EARLY):
        early_side(i).wait_recv()
        early_out.append(pltpu.make_async_copy(from_side.at[i], g_out.at[i], out_sem.at[5 + i]))
        early_out[i].start()
    for i in range(EARLY):
        early_core(i).wait_send()
        early_side(i).wait_send()

    for c in (keys_out, values_out, query_out, wh_out, wdz_out, *early_out):
        c.wait()


def forward(tok, qkv, memory, rate_w, forget, R, H, n_seq, n_head, lr_scale):
    count, width = tok.shape
    F = qkv.shape[2]
    chips, wide = n_seq // 2, 2 * R
    FB = F // wide
    assert n_seq % 4 == 0 and n_seq >= 16 and FB * wide == F and chips * wide == width
    anywhere = pl.BlockSpec(memory_space=pl.ANY)
    vmem = pl.BlockSpec(memory_space=pltpu.VMEM)
    S = jax.ShapeDtypeStruct
    dma = pltpu.SemaphoreType.DMA
    return pl.pallas_call(
        functools.partial(forward_kernel, n_seq, n_head, lr_scale),
        out_shape=(
            S((2, chips, count, wide), BF16),
            S((2, count, H), BF16),
            S((FB, count, wide), BF16),
            S((FB, count, wide), BF16),
            S((chips, count, wide), BF16),
            S((EARLY, R, H), BF16),
        ),
        in_specs=[anywhere, anywhere, anywhere, vmem, vmem],
        out_specs=(anywhere,) * 6,
        scratch_shapes=[
            pltpu.VMEM(tok.shape, BF16),
            pltpu.VMEM(memory.shape, F32),
            pltpu.VMEM((2, R, H), BF16),
            pltpu.VMEM((2, chips, wide, H), BF16),
            pltpu.VMEM((2, width, F), BF16),
            pltpu.VMEM((chips, count, wide), BF16),
            pltpu.VMEM((chips, count, wide), BF16),
            pltpu.VMEM((FB, count, wide), BF16),
            pltpu.VMEM((count, H), F32),
            pltpu.VMEM((count, H), F32),
            pltpu.VMEM((count, H), BF16),
            pltpu.VMEM((count, H), BF16),
            pltpu.VMEM((count, H), BF16),
            pltpu.VMEM((n_head, chips, count, wide), BF16),
            pltpu.VMEM((chips, count, wide), BF16),
            pltpu.VMEM((count, 1), F32),
            pltpu.VMEM((n_seq, 1, count), F32),
            pltpu.VMEM((EARLY, wide, H), BF16),
            pltpu.VMEM((EARLY, R, H), BF16),
            pltpu.VMEM((EARLY, R, H), BF16),
            dma((2, 4, chips, PIECES)),
            dma((2, n_seq, PIECES)),
            dma((n_seq,)),
            dma((n_seq,)),
            dma((2, max(n_head - 1, 1), FB)),
            dma((2, chips)),
            dma((max(n_head - 1, 1), chips)),
            dma((n_head, chips)),
            dma((3,)),
            dma((5 + EARLY,)),
            dma((2, chips)),
            dma((2, EARLY)),
            dma((2, EARLY)),
            dma,
            dma,
        ],
        compiler_params=pltpu.CompilerParams(
            collective_id=0, has_side_effects=True, vmem_limit_bytes=VMEM_LIMIT
        ),
    )(tok, qkv, memory, rate_w, forget)


def backward_kernel(
    n_seq, n_head,
    xx_in, yy_in, q_in, v_in, recall_in, g_in, persist_in,
    grad, attended,
    persist, xx, yy, query, values, recall, got, recalled, G, from_core, from_side, from_left, from_right, acc,
    c_send, c_recv, s_send, s_recv, z_send, l_recv, r_recv, x_send, x_recv, in_sem,
):
    me = Place(n_seq, n_head)
    L, line, side, core, head = me.length, me.line, me.side, me.core, me.head
    count, wide = xx.shape[2], xx.shape[3]
    R, H = acc.shape
    FB = query.shape[0]
    base = head * FB
    peers = me.peers()

    pairs = (
        (recall_in, recall), (xx_in.at[1], xx.at[1]), (yy_in.at[1], yy.at[1]), (xx_in.at[0], xx.at[0]),
        (yy_in.at[0], yy.at[0]), (q_in, query), (v_in, values), (persist_in, persist),
        *[(g_in.at[i], from_side.at[1, me.order(i)]) for i in range(EARLY)],
    )
    loads = [pltpu.make_async_copy(a, b, in_sem.at[i]) for i, (a, b) in enumerate(pairs)]
    for c in (loads[1], loads[2], loads[0], *loads[3:]):
        c.start()

    barrier = pltpu.get_barrier_semaphore()

    def greet(where):
        pl.semaphore_signal(barrier, inc=1, device_id=where, device_id_type=MESH)

    greet(me.at(line, side, 1 - core))
    greet(me.at(line, 1 - side, core))

    @pl.when(line > 0)
    def _():
        greet(me.at(line - 1, side, core))

    @pl.when(line < L - 1)
    def _():
        greet(me.at(line + 1, side, core))

    for peer in peers:
        greet(peer)
    ends = jnp.where(line > 0, 1, 0) + jnp.where(line < L - 1, 1, 0)
    pl.semaphore_wait(barrier, 2 + n_head - 1 + ends)

    def rcopy(b, p):
        there = peers[p]["head"] * FB
        return remote(recall.at[there + b], got.at[head, b], x_send.at[p, b], x_recv.at[head, b], peers[p])

    loads[0].wait()

    @pl.loop(0, FB)
    def _(b):
        for p in range(n_head - 1):
            rcopy(b, p).start()

    for c in loads[1:3]:
        c.wait()

    mine = pl.ds(pl.multiple_of(core * R, R), R)
    theirs = pl.ds(pl.multiple_of((1 - core) * R, R), R)

    def core_copy(w, j):
        return remote(
            G.at[w, j, theirs, :], from_core.at[w, j], c_send.at[w, j], c_recv.at[w, j],
            me.at(line, side, 1 - core),
        )

    def side_copy(w, l):
        return remote(
            G.at[w, l * 2 + 1 - side, mine, :], from_side.at[w, l], s_send.at[w, l], s_recv.at[w, l],
            me.at(line, 1 - side, core),
        )

    def right_copy(w, l):
        return remote(
            G.at[w, l * 2 + side, mine, :], from_left.at[w, l], z_send.at[w, l], l_recv.at[w, l],
            me.at(line + 1, side, core),
        )

    def left_copy(w, l):
        return remote(
            G.at[w, l * 2 + side, mine, :], from_right.at[w, l], z_send.at[w, l], r_recv.at[w, l],
            me.at(line - 1, side, core),
        )

    def partial(w, j):
        G[w, j] = dot_tn(xx[w, j], yy[w]).astype(BF16)
        core_copy(w, j).start()

    there = 2 * L - EARLY
    far = L - 1
    at_end = (line == 0) | (line == L - 1)
    low = jnp.logical_not(at_end) & (line < L // 2)

    def across(n):
        both = 2 * (L - EARLY)
        n = jnp.where(low & (n == both - 1), both, jnp.where(low & (n == both), both - 1, n))
        w = jnp.where(n < both, 1 - n % 2, 0)
        return w, me.order(jnp.where(n < both, L - 1 - n // 2, EARLY - 1 - (n - both)))

    def along(n):
        t = n - (2 * far - 4)
        last_low = 2 * far - 4 + jnp.where(t % 2 == 0, 2 + t // 2, t // 2)
        last_high = 2 * far - 4 + (t % 2) * 2 + t // 2
        inner = jnp.where(t < 0, n, jnp.where(low, last_low, last_high))
        outer = jnp.where(n == 0, 2 * far - 2, jnp.where(n == 2 * far - 1, n, n - 1))
        q = jnp.where(at_end, outer, inner)
        own = n >= 2 * far
        return jnp.where(own, 1 - (n - 2 * far), 1 - q % 2), jnp.where(own, 0, L - 1 - q // 2)

    def line_partial(n):
        w, i = along(n)
        partial(w, me.order(i) * 2 + side)

    def line_finish(n):
        w, i = along(n)
        l = me.order(i)
        j = l * 2 + side
        core_copy(w, j).wait_recv()

        @pl.when((w == 0) | (i >= EARLY))
        def _():
            remote(
                from_side.at[w, l], from_side.at[w, l], s_send.at[w, l], s_recv.at[w, l],
                me.at(line, 1 - side, core),
            ).wait_recv()

        acc[...] = G[w, j, mine, :].astype(F32) + from_core[w, j].astype(F32) + from_side[w, l].astype(F32)

        @pl.when((l >= line) & (line > 0))
        def _():
            remote(
                from_left.at[w, l], from_left.at[w, l], z_send.at[w, l], l_recv.at[w, l],
                me.at(line - 1, side, core),
            ).wait_recv()
            acc[...] += from_left[w, l].astype(F32)

        @pl.when((l <= line) & (line < L - 1))
        def _():
            remote(
                from_right.at[w, l], from_right.at[w, l], z_send.at[w, l], r_recv.at[w, l],
                me.at(line + 1, side, core),
            ).wait_recv()
            acc[...] += from_right[w, l].astype(F32)

        @pl.when(l == line)
        def _():
            for tile in range(H // LANES):
                rows = pl.ds(tile * 2 + w, R, stride=2 * H // LANES)
                grad[rows, :] = acc[:, tile * LANES : (tile + 1) * LANES]

        @pl.when(l != line)
        def _():
            G[w, j, mine, :] = acc[...].astype(BF16)

        @pl.when(l > line)
        def _():
            right_copy(w, l).start()

        @pl.when(l < line)
        def _():
            left_copy(w, l).start()

    @pl.when(at_end)
    def _():
        line_partial(0)

    @pl.loop(0, there + 1)
    def _(n):
        @pl.when(n == 1)
        def _():
            loads[3].wait()
            loads[4].wait()

        @pl.when(n < there)
        def _():
            w, l = across(n)
            partial(w, l * 2 + 1 - side)

        @pl.when(n > 0)
        def _():
            w, l = across(n - 1)
            j = l * 2 + 1 - side
            core_copy(w, j).wait_recv()
            both = G[w, j, mine, :].astype(F32) + from_core[w, j].astype(F32)
            G[w, j, mine, :] = both.astype(BF16)
            side_copy(w, l).start()

        @pl.when(n == 2)
        def _():
            for c in loads[8:]:
                c.wait()

        @pl.when((n == 2) & at_end)
        def _():
            line_finish(0)

    for c in loads[5:8]:
        c.wait()

    heads_here = FB * wide // HEAD_DIM
    per = wide // HEAD_DIM
    chunk = count // 2
    scale = HEAD_DIM ** (-0.5)
    persist_count = persist.shape[1]

    def attend(n):
        b = n // per
        cols = pl.ds(pl.multiple_of((n % per) * HEAD_DIM, HEAD_DIM), HEAD_DIM)
        flat = pl.ds(pl.multiple_of(n * HEAD_DIM, HEAD_DIM), HEAD_DIM)
        for part in range(2):
            seen = (part + 1) * chunk
            q = query[b, pl.ds(part * chunk, chunk), cols]
            row = lax.broadcasted_iota(jnp.int32, (chunk, seen), 0) + part * chunk
            visible = lax.broadcasted_iota(jnp.int32, (chunk, seen), 1) <= row
            rec = recalled[b, pl.ds(0, seen), cols]
            key = xx[0, base + b, pl.ds(0, seen), cols]
            val = values[b, pl.ds(0, seen), cols]
            s0 = dot_nt(q, persist[0, :, flat]) * scale
            s1 = jnp.where(visible, dot_nt(q, rec) * scale, -1e30)
            s2 = jnp.where(visible, dot_nt(q, key) * scale, -1e30)
            top = jnp.maximum(
                jnp.max(s0, axis=1, keepdims=True),
                jnp.maximum(jnp.max(s1, axis=1, keepdims=True), jnp.max(s2, axis=1, keepdims=True)),
            )
            e0, e1, e2 = jnp.exp(s0 - top), jnp.exp(s1 - top), jnp.exp(s2 - top)
            norm = 1.0 / (
                jnp.sum(e0, axis=1, keepdims=True)
                + jnp.sum(e1, axis=1, keepdims=True)
                + jnp.sum(e2, axis=1, keepdims=True)
            )
            out = dot((e0 * norm).astype(BF16), persist[1, :, flat])
            out = out + dot((e1 * norm).astype(BF16), rec)
            out = out + dot((e2 * norm).astype(BF16), val)
            attended[pl.ds(part * chunk, chunk), flat] = out.astype(BF16)

    def recall_all():
        @pl.loop(0, FB)
        def _(b):
            total = recall[base + b].astype(F32)
            for by in range(1, n_head):
                other = (head + by) % n_head
                remote(
                    got.at[other, b], got.at[other, b], x_send.at[0, b], x_recv.at[other, b], peers[0]
                ).wait_recv()
                total = total + got[other, b].astype(F32)
            recalled[b] = total.astype(BF16)

    each = -(-heads_here // 2)

    def sent():
        @pl.loop(0, FB)
        def _(b):
            for p in range(n_head - 1):
                rcopy(b, p).wait_send()

        @pl.loop(0, there)
        def _(n):
            w, l = across(n)
            core_copy(w, l * 2 + 1 - side).wait_send()
            side_copy(w, l).wait_send()

    @pl.loop(jnp.where(at_end, 1, 0), 2 * L)
    def _(n):
        line_partial(n)

        @pl.when(n == 2 * L - 1)
        def _():
            sent()

        @pl.when(n == far)
        def _():
            recall_all()

        @pl.loop(jnp.maximum((n - far) * each, 0), jnp.clip((n - far + 1) * each, 0, heads_here))
        def _(k):
            attend(k)

        line_finish(n)

    @pl.loop(0, L)
    def _(l):
        for w in range(2):
            core_copy(w, l * 2 + side).wait_send()

            @pl.when(l > line)
            def _():
                right_copy(w, l).wait_send()

            @pl.when(l < line)
            def _():
                left_copy(w, l).wait_send()


def backward(xx, yy, query, values, recall, early, persist, n_seq, n_head, R):
    _, chips, count, wide = xx.shape
    H, FB = yy.shape[2], query.shape[0]
    L = n_seq // 4
    anywhere = pl.BlockSpec(memory_space=pl.ANY)
    vmem = pl.BlockSpec(memory_space=pltpu.VMEM)
    S = jax.ShapeDtypeStruct
    dma = pltpu.SemaphoreType.DMA
    return pl.pallas_call(
        functools.partial(backward_kernel, n_seq, n_head),
        out_shape=(S((R * 2 * H // LANES, LANES), F32), S((count, FB * wide), BF16)),
        in_specs=[anywhere] * 7,
        out_specs=(vmem, vmem),
        scratch_shapes=[
            pltpu.VMEM(persist.shape, BF16),
            pltpu.VMEM((2, chips, count, wide), BF16),
            pltpu.VMEM((2, count, H), BF16),
            pltpu.VMEM((FB, count, wide), BF16),
            pltpu.VMEM((FB, count, wide), BF16),
            pltpu.VMEM((chips, count, wide), BF16),
            pltpu.VMEM((n_head, FB, count, wide), BF16),
            pltpu.VMEM((FB, count, wide), BF16),
            pltpu.VMEM((2, chips, wide, H), BF16),
            pltpu.VMEM((2, chips, R, H), BF16),
            pltpu.VMEM((2, L, R, H), BF16),
            pltpu.VMEM((2, L, R, H), BF16),
            pltpu.VMEM((2, L, R, H), BF16),
            pltpu.VMEM((R, H), F32),
            dma((2, chips)),
            dma((2, chips)),
            dma((2, L)),
            dma((2, L)),
            dma((2, L)),
            dma((2, L)),
            dma((2, L)),
            dma((max(n_head - 1, 1), FB)),
            dma((n_head, FB)),
            dma((8 + EARLY,)),
        ],
        compiler_params=pltpu.CompilerParams(
            collective_id=1, has_side_effects=True, vmem_limit_bytes=VMEM_LIMIT
        ),
    )(xx, yy, query, values, recall, early, persist)


def interleave(x):
    R, two, H = x.shape
    return x.reshape(R, two, H // LANES, LANES).transpose(0, 2, 1, 3).reshape(R * two * H // LANES, LANES)


def layered(x, R, H):
    return x.reshape(R, H // LANES, 2, LANES).transpose(0, 2, 1, 3).reshape(R, 2, H)


def update_kernel(decay, share, grad, memory, momentum, memory_out, momentum_out):
    new = decay[0] * momentum[...] - grad[...]
    momentum_out[...] = new
    memory_out[...] = (1.0 - share[0]) * memory[...] + new


def update(decay, share, grad, memory, momentum):
    rows = grad.shape[0]
    smem = pl.BlockSpec(memory_space=pltpu.SMEM)
    flat = pl.BlockSpec((rows // UPDATE_STEPS, LANES), lambda i: (i, 0))
    out = jax.ShapeDtypeStruct(grad.shape, F32)
    return pl.pallas_call(
        update_kernel,
        grid=(UPDATE_STEPS,),
        out_shape=(out, out),
        in_specs=[smem, smem, flat, flat, flat],
        out_specs=(flat, flat),
    )(decay, share, grad, memory, momentum)


def on_device(
    tokens, qkv_weight, persistent, rate_weight, forget_rate, momentum_decay, forget_share, memory, momentum
):
    n_seq, n_head = lax.axis_size("seq"), lax.axis_size("head")
    seg_len, width = tokens.shape[1], tokens.shape[2]
    lr_scale = 2.0 / (width * n_seq * seg_len) ** 0.5
    R, _, H = memory.shape
    memory_tiles = interleave(memory)
    qkv = jnp.transpose(qkv_weight, (1, 0, 2))
    xx, yy, query, values, recall, early = forward(
        tokens[0], qkv, memory_tiles, rate_weight[None], forget_rate, R, H, n_seq, n_head, lr_scale
    )
    grad, attended = backward(xx, yy, query, values, recall, early, persistent, n_seq, n_head, R)
    memory, momentum = update(momentum_decay, forget_share, grad, memory_tiles, interleave(momentum))
    memory, momentum = layered(memory, R, H), layered(momentum, R, H)
    return (attended[None], memory, momentum)


def solution(mesh):
    placed = (
        P(None, "seq", None),
        P(None, None, "head"),
        P(None, None, "head"),
        P(),
        P(None, "seq"),
        P(),
        P(),
        P("seq", None, "head"),
        P("seq", None, "head"),
    )
    return jax.shard_map(
        on_device,
        mesh=mesh,
        in_specs=placed,
        out_specs=(P(None, "seq", "head"), P("seq", None, "head"), P("seq", None, "head")),
        check_vma=False,
    )
```

```python
import functools

import jax
import jax.numpy as jnp
from jax import lax
from jax.experimental import pallas as pl
from jax.experimental.pallas import tpu as pltpu
from jax.sharding import PartitionSpec as P

HEAD_DIM = 128
LANES = 128
MESH = pl.DeviceIdType.MESH
VMEM_LIMIT = 67043328
PIECES = 2
EARLY = 2
UPDATE_STEPS = 2
F32, BF16 = jnp.float32, jnp.bfloat16


def remote(src, dst, send_sem, recv_sem, where):
    return pltpu.make_async_remote_copy(
        src_ref=src,
        dst_ref=dst,
        send_sem=send_sem,
        recv_sem=recv_sem,
        device_id=where,
        device_id_type=MESH,
    )


def dot(a, b):
    return jnp.dot(a, b, preferred_element_type=F32)


def dot_nt(a, b):
    return lax.dot_general(a, b, (((1,), (1,)), ((), ())), preferred_element_type=F32)


def dot_tn(a, b):
    return lax.dot_general(a, b, (((0,), (0,)), ((), ())), preferred_element_type=F32)


class Place:
    def __init__(self, n_seq, n_head):
        self.n_seq, self.n_head = n_seq, n_head
        self.length = n_seq // 4
        self.seq, self.head = lax.axis_index("seq"), lax.axis_index("head")
        self.line = self.seq // 4
        self.side = (self.seq // 2) % 2
        self.core = self.seq % 2

    def at(self, line, side, core):
        return {"seq": (line * 2 + side) * 2 + core}

    def order(self, i):
        left, right = self.line, self.length - 1 - self.line
        both = jnp.minimum(left, right)
        paired = i <= 2 * both
        step = jnp.where(paired, (i + 1) // 2, i - both)
        to_left = jnp.where(paired, i % 2 == 1, left > right)
        return jnp.where(to_left, self.line - step, self.line + step)

    def peers(self):
        return [{"head": (self.head + by) % self.n_head} for by in range(1, self.n_head)]


def rows_loop(total, step, body):
    @pl.loop(0, total // step)
    def _(i):
        body(pl.ds(pl.multiple_of(i * step, step), step))


def forward_kernel(
    n_seq, n_head, lr_scale,
    tok_in, qkv, memory, rate_w, forget,
    xx_out, yy_out, q_out, v_out, recall_out, g_out,
    tok, staged, own, W, wbuf, keys, query, values, zk, zz, hk, hq, wh, errs, recall, weight, frb, G, from_core, from_side,
    w_send, w_recv, f_send, f_recv, k_send, k_recv, e_send, e_recv, qkv_sem, out_sem, block_sem, g_send, g_recv, mem_sem, tok_sem,
):
    me = Place(n_seq, n_head)
    L, line, side, core, head = me.length, me.line, me.side, me.core, me.head
    chips = n_seq // 2
    count, width = tok.shape
    R, H = own.shape[1:]
    wide = 2 * R
    FB = values.shape[0]
    base = head * FB
    peers = me.peers()

    memory_load = pltpu.make_async_copy(memory, staged, mem_sem)
    memory_load.start()
    tok_load = pltpu.make_async_copy(tok_in, tok, tok_sem)
    loads = [pltpu.make_async_copy(qkv.at[k], wbuf.at[s], qkv_sem.at[k]) for k, s in ((1, 0), (0, 1), (2, 0))]
    tok_load.start()
    loads[0].start()
    loads[1].start()

    barrier = pltpu.get_barrier_semaphore()
    for by in range(1, n_seq):
        pl.semaphore_signal(barrier, inc=1, device_id={"seq": (me.seq + by) % n_seq}, device_id_type=MESH)
    for peer in peers:
        pl.semaphore_signal(barrier, inc=1, device_id=peer, device_id_type=MESH)
    def cast(k):
        for tile in range(H // LANES):
            tiles = staged[pl.ds(tile * 2 + k, R, stride=2 * H // LANES), :]
            own[k, :, tile * LANES : (tile + 1) * LANES] = tiles.astype(BF16)

    memory_load.wait()
    cast(0)
    pl.semaphore_wait(barrier, n_seq - 1 + n_head - 1)

    piece = R // PIECES

    def block(w, l, m, c, p):
        return W.at[w, l * 2 + m, pl.ds(pl.multiple_of(c * R + p * piece, piece), piece), :]

    def copy(w, l, m, c, p, way, mine=False):
        where = (
            me.at(line + 1, side, core),
            me.at(line - 1, side, core),
            me.at(line, 1 - side, core),
            me.at(line, side, 1 - core),
        )[way]
        dst = block(w, l, m, c, p)
        src = own.at[w, pl.ds(pl.multiple_of(p * piece, piece), piece), :] if mine else dst
        chip = l * 2 + m
        return remote(src, dst, w_send.at[w, way, chip, p], w_recv.at[w, chip * 2 + c, p], where)

    def spread(w, l, p, act, ways=(0, 1, 2, 3), mine=False):
        if 0 in ways:

            @pl.when((l <= line) & (line < L - 1))
            def _():
                act(copy(w, l, side, core, p, 0, mine))

        if 1 in ways:

            @pl.when((l >= line) & (line > 0))
            def _():
                act(copy(w, l, side, core, p, 1, mine))

        for way in (2, 3):
            if way in ways:
                act(copy(w, l, side, core, p, way, mine))

    def start(c):
        c.start()

    def arrived(w, l, m, c, p):
        copy(w, l, m, c, p, 2).wait_recv()

    def start_own(w, ways):
        for p in range(PIECES):
            spread(w, line, p, start, ways, True)

    for p in range(PIECES):
        spread(0, line, p, start, (0, 1, 3), True)
    spread(0, line, 0, start, (2,), True)
    cast(1)
    fcopies = []
    for by in range(1, n_seq):
        fcopies.append(
            remote(forget, frb.at[me.seq], f_send.at[by], f_recv.at[me.seq], {"seq": (me.seq + by) % n_seq})
        )
    for c in fcopies:
        c.start()
    frb[me.seq] = forget[...]

    def xcopy(which, buf, b, p):
        return remote(
            buf.at[base + b], buf.at[base + b], k_send.at[which, p, b], k_recv.at[which, base + b], peers[p]
        )

    def project(slot, b):
        cols = pl.ds(pl.multiple_of(b * wide, wide), wide)
        return dot(tok[...], wbuf[slot, :, cols]).astype(BF16)

    def project_shared(which, buf, slot):
        loads[which].wait()

        @pl.loop(0, FB)
        def _(b):
            buf[base + b] = project(slot, b)
            for p in range(n_head - 1):
                xcopy(which, buf, b, p).start()

    def project_values():
        loads[2].wait()

        @pl.loop(0, FB)
        def _(b):
            values[b] = project(0, b)

    def weigh(rows, start_row, later):
        x = tok[rows, :].astype(F32)
        rate = jnp.sum(x * rate_w[...], axis=1, keepdims=True)
        n = x.shape[0]
        t = lax.broadcasted_iota(jnp.int32, (n, count), 0) + start_row
        u = lax.broadcasted_iota(jnp.int32, (n, count), 1)
        tail = jnp.sum(jnp.where(u > t, forget[...], 0.0), axis=1, keepdims=True) + later
        weight[rows, :] = lr_scale * jax.nn.sigmoid(rate) * jnp.exp(-tail)

    def weigh_all():
        for by in range(1, n_seq):
            other = (me.seq + by) % n_seq
            remote(forget, frb.at[other], f_send.at[by], f_recv.at[other], {"seq": other}).wait_recv()
        totals = jnp.sum(frb[...], axis=2, keepdims=True)
        which_seq = lax.broadcasted_iota(jnp.int32, totals.shape, 0)
        later = jnp.sum(jnp.where(which_seq > me.seq, totals, 0.0), axis=(0, 1, 2), keepdims=True)[0]

        @pl.loop(0, count // 32)
        def _(i):
            weigh(pl.ds(pl.multiple_of(i * 32, 32), 32), i * 32, later)

    for w in range(2):
        W[w, line * 2 + side, pl.ds(pl.multiple_of(core * R, R), R), :] = own[w]
    zk[...] = jnp.zeros_like(zk)
    right = L - 1 - line

    def keys_ready(which, buf, j):
        @pl.when((j < base) | (j >= base + FB))
        def _():
            remote(buf.at[j], buf.at[j], k_send.at[which, 0, 0], k_recv.at[which, j], peers[0]).wait_recv()

    def chip(l, mm):
        return l * 2 + jnp.where(mm == 0, side, 1 - side)

    def other_core(w, l, mm):
        for p in range(PIECES):
            arrived(w, l, jnp.where(mm == 0, side, 1 - side), 1 - core, p)

    def ecopy(j, p):
        return remote(errs.at[head, j], errs.at[head, j], e_send.at[p, j], e_recv.at[head, j], peers[p])

    def move(k):
        def come(away, step, ways):
            each = away * PIECES

            @pl.when((k > 0) & (k <= 2 * each))
            def _():
                at = k - 1
                w = jnp.where(at >= each, 1, 0)
                at = at - w * each
                l = line + step * (1 + at // PIECES)
                arrived(w, l, side, core, at % PIECES)
                spread(w, l, at % PIECES, start, ways)

            @pl.when(k == each)
            def _():
                start_own(1, ways[:1])

        come(line, -1, (0, 3))
        come(right, 1, (1, 3))

        @pl.when(k == 1)
        def _():
            start_own(1, (3,))

        total = 2 * L * PIECES

        def entry(n):
            return n // (L * PIECES), me.order(n // PIECES % L), n % PIECES

        half = L * PIECES
        first = k + jnp.where(k < half, 1, 2)
        end = jnp.minimum(k + jnp.where(k < half - 1, 2, 3), total)

        @pl.loop(first, end)
        def _(n):
            w, l, p = entry(n)

            @pl.when(l == line)
            def _():
                spread(w, l, p, start, (2,), True)

            @pl.when(l != line)
            def _():
                spread(w, l, p, start, (2,))

        @pl.when((k > 0) & (k <= total))
        def _():
            w, l, p = entry(k - 1)
            arrived(w, l, 1 - side, core, p)
            copy(w, l, 1 - side, core, p, 3).start()

    def hide(rows):
        z = zk[rows, :]
        s = jax.nn.sigmoid(z)
        hid = (z * s).astype(BF16)
        hk[rows, :] = hid
        wh[rows, :] = (weight[rows, :] * hid.astype(F32)).astype(BF16)
        zk[rows, :] = weight[rows, :] * (s * (1.0 + z * (1.0 - s)))

    def hide_query(rows):
        hq[rows, :] = jax.nn.silu(zz[rows, :]).astype(BF16)

    keys_out = pltpu.make_async_copy(keys, xx_out.at[0], out_sem.at[0])
    values_out = pltpu.make_async_copy(values, v_out, out_sem.at[1])
    query_out = pltpu.make_async_copy(query.at[pl.ds(base, FB)], q_out, out_sem.at[2])
    wh_out = pltpu.make_async_copy(wh, yy_out.at[1], out_sem.at[3])

    def err_copy(j):
        return pltpu.make_async_copy(errs.at[head, j], xx_out.at[1, j], block_sem.at[0, j])

    def recall_copy(j):
        return pltpu.make_async_copy(recall.at[j], recall_out.at[j], block_sem.at[1, j])

    def add_first(i):
        @pl.loop(0, 2)
        def _(mm):
            l = me.order(i)
            other_core(0, l, mm)
            j = chip(l, mm)
            keys_ready(0, keys, j)
            zk[...] += dot(keys[j], W[0, j])

    def make_error(i, mm):
        @pl.when((i >= 0) & (i < L))
        def _():
            l = me.order(i)
            other_core(1, l, mm)
            j = chip(l, mm)
            part = dot_nt(hk[...], W[1, j])
            mine = (j >= base) & (j < base + FB)

            @pl.when(mine)
            def _():
                errs[head, j] = (part - values[j - base].astype(F32)).astype(BF16)

            @pl.when(jnp.logical_not(mine))
            def _():
                errs[head, j] = part.astype(BF16)

            for p in range(n_head - 1):
                ecopy(j, p).start()

    def make_recall(i):
        @pl.loop(0, 2)
        def _(mm):
            j = chip(me.order(i), mm)
            recall[j] = dot_nt(hq[...], W[1, j]).astype(BF16)
            recall_copy(j).start()

    def pull_error(i, mm):
        @pl.when((i >= 0) & (i < L))
        def _():
            j = chip(me.order(i), mm)
            for by in range(1, n_head):
                other = (head + by) % n_head
                remote(
                    errs.at[other, j], errs.at[other, j], e_send.at[0, j], e_recv.at[other, j], peers[0]
                ).wait_recv()
            total = errs[0, j].astype(F32)
            for p in range(1, n_head):
                total = total + errs[p, j].astype(F32)
            for p in range(n_head - 1):
                ecopy(j, p).wait_send()
            errs[head, j] = total.astype(BF16)
            err_copy(j).start()
            zz[...] += dot(errs[head, j], W[1, j])

    mine = pl.ds(pl.multiple_of(core * R, R), R)
    theirs = pl.ds(pl.multiple_of((1 - core) * R, R), R)

    def early_core(i):
        return remote(
            G.at[i, theirs, :], from_core.at[i], g_send.at[0, i], g_recv.at[0, i], me.at(line, side, 1 - core)
        )

    def early_side(i):
        return remote(
            G.at[i, mine, :], from_side.at[i], g_send.at[1, i], g_recv.at[1, i], me.at(line, 1 - side, core)
        )

    def early_partial(i):
        G[i] = dot_tn(errs[head, chip(me.order(i), 1)], wh[...]).astype(BF16)
        early_core(i).start()

    def early_on(i):
        early_core(i).wait_recv()
        G[i, mine, :] = (G[i, mine, :].astype(F32) + from_core[i].astype(F32)).astype(BF16)
        early_side(i).start()

    def add_query(low, high):
        @pl.loop(low, high)
        def _(j):
            keys_ready(1, query, j)
            zz[...] += dot(query[j], W[0, j])

    @pl.loop(0, PIECES * (2 * L + 1) + 1)
    def _(k):
        move(k)
        slot = k // PIECES
        even = k % PIECES == 0
        last = k % PIECES == PIECES - 1

        @pl.when(k == 0)
        def _():
            tok_load.wait()
            project_shared(0, keys, 0)
            loads[2].start()

        @pl.when(k == 1)
        def _():
            project_shared(1, query, 1)

        @pl.when(k == PIECES)
        def _():
            project_values()

        @pl.when(k == PIECES + 1)
        def _():
            weigh_all()

        @pl.when(even & (slot > 0) & (slot <= L))
        def _():
            add_first(slot - 1)

        @pl.when(k == PIECES * L)
        def _():
            keys_out.start()
            rows_loop(count, 16, hide)
            wh_out.start()
            zz[...] = jnp.zeros_like(zz)

        @pl.when(even & (slot >= L) & (slot <= 2 * L))
        def _():
            @pl.loop(jnp.where(slot == L, -1, 0), 2)
            def _(nth):
                mm = jnp.maximum(nth, 0)
                make_error(slot - L + jnp.where(nth < 0, 0, 1 - 2 * mm), mm)

        @pl.when(k == PIECES * L + 1)
        def _():
            add_query(0, chips // 2)

        @pl.when(k == PIECES * (L + 1) + 1)
        def _():
            add_query(chips // 2, chips)
            rows_loop(count, 16, hide_query)
            zz[...] = jnp.zeros_like(zz)
            values_out.start()
            query_out.start()

        @pl.when(last & (slot > L) & (slot <= 2 * L))
        def _():
            make_recall(slot - L - 1)

        @pl.when((last & (slot > L)) | (k == PIECES * (2 * L + 1)))
        def _():
            @pl.loop(jnp.where(slot == L + 1, -1, 0), 2)
            def _(nth):
                mm = jnp.maximum(nth, 0)
                pull_error(slot - L - jnp.where(nth < 0, 1, 2 * mm), mm)

        @pl.when(even & (slot > 2 * L - 2) & (slot <= 2 * L - 2 + EARLY))
        def _():
            early_on(slot - 2 * L + 1)

        @pl.when(last & (slot > 2 * L - 3) & (slot <= 2 * L - 3 + EARLY))
        def _():
            early_partial(slot - 2 * L + 2)


    def pull(rows):
        hk[rows, :] = (zz[rows, :] * zk[rows, :]).astype(BF16)

    rows_loop(count, 16, pull)
    wdz_out = pltpu.make_async_copy(hk, yy_out.at[0], out_sem.at[4])
    wdz_out.start()

    for c in fcopies:
        c.wait_send()

    @pl.loop(0, FB)
    def _(b):
        for which, buf in enumerate((keys, query)):
            for p in range(n_head - 1):
                xcopy(which, buf, b, p).wait_send()

    @pl.loop(0, L)
    def _(l):
        for w in range(2):
            for p in range(PIECES):
                spread(w, l, p, lambda c: c.wait_send())
                copy(w, l, 1 - side, core, p, 3).wait_send()

    @pl.loop(0, chips)
    def _(j):
        err_copy(j).wait()
        recall_copy(j).wait()

    early_out = []
    for i in range(EARLY):
        early_side(i).wait_recv()
        early_out.append(pltpu.make_async_copy(from_side.at[i], g_out.at[i], out_sem.at[5 + i]))
        early_out[i].start()
    for i in range(EARLY):
        early_core(i).wait_send()
        early_side(i).wait_send()

    for c in (keys_out, values_out, query_out, wh_out, wdz_out, *early_out):
        c.wait()


def forward(tok, qkv, memory, rate_w, forget, R, H, n_seq, n_head, lr_scale):
    count, width = tok.shape
    F = qkv.shape[2]
    chips, wide = n_seq // 2, 2 * R
    FB = F // wide
    assert n_seq % 4 == 0 and n_seq >= 16 and FB * wide == F and chips * wide == width
    anywhere = pl.BlockSpec(memory_space=pl.ANY)
    vmem = pl.BlockSpec(memory_space=pltpu.VMEM)
    S = jax.ShapeDtypeStruct
    dma = pltpu.SemaphoreType.DMA
    return pl.pallas_call(
        functools.partial(forward_kernel, n_seq, n_head, lr_scale),
        out_shape=(
            S((2, chips, count, wide), BF16),
            S((2, count, H), BF16),
            S((FB, count, wide), BF16),
            S((FB, count, wide), BF16),
            S((chips, count, wide), BF16),
            S((EARLY, R, H), BF16),
        ),
        in_specs=[anywhere, anywhere, anywhere, vmem, vmem],
        out_specs=(anywhere,) * 6,
        scratch_shapes=[
            pltpu.VMEM(tok.shape, BF16),
            pltpu.VMEM(memory.shape, F32),
            pltpu.VMEM((2, R, H), BF16),
            pltpu.VMEM((2, chips, wide, H), BF16),
            pltpu.VMEM((2, width, F), BF16),
            pltpu.VMEM((chips, count, wide), BF16),
            pltpu.VMEM((chips, count, wide), BF16),
            pltpu.VMEM((FB, count, wide), BF16),
            pltpu.VMEM((count, H), F32),
            pltpu.VMEM((count, H), F32),
            pltpu.VMEM((count, H), BF16),
            pltpu.VMEM((count, H), BF16),
            pltpu.VMEM((count, H), BF16),
            pltpu.VMEM((n_head, chips, count, wide), BF16),
            pltpu.VMEM((chips, count, wide), BF16),
            pltpu.VMEM((count, 1), F32),
            pltpu.VMEM((n_seq, 1, count), F32),
            pltpu.VMEM((EARLY, wide, H), BF16),
            pltpu.VMEM((EARLY, R, H), BF16),
            pltpu.VMEM((EARLY, R, H), BF16),
            dma((2, 4, chips, PIECES)),
            dma((2, n_seq, PIECES)),
            dma((n_seq,)),
            dma((n_seq,)),
            dma((2, max(n_head - 1, 1), FB)),
            dma((2, chips)),
            dma((max(n_head - 1, 1), chips)),
            dma((n_head, chips)),
            dma((3,)),
            dma((5 + EARLY,)),
            dma((2, chips)),
            dma((2, EARLY)),
            dma((2, EARLY)),
            dma,
            dma,
        ],
        compiler_params=pltpu.CompilerParams(
            collective_id=0, has_side_effects=True, vmem_limit_bytes=VMEM_LIMIT
        ),
    )(tok, qkv, memory, rate_w, forget)


def backward_kernel(
    n_seq, n_head,
    xx_in, yy_in, q_in, v_in, recall_in, g_in, persist_in,
    grad, attended,
    persist, xx, yy, query, values, recall, got, recalled, G, from_core, from_side, from_left, from_right, acc,
    c_send, c_recv, s_send, s_recv, z_send, l_recv, r_recv, x_send, x_recv, in_sem,
):
    me = Place(n_seq, n_head)
    L, line, side, core, head = me.length, me.line, me.side, me.core, me.head
    count, wide = xx.shape[2], xx.shape[3]
    R, H = acc.shape
    FB = query.shape[0]
    base = head * FB
    peers = me.peers()

    pairs = (
        (recall_in, recall), (xx_in.at[1], xx.at[1]), (yy_in.at[1], yy.at[1]), (xx_in.at[0], xx.at[0]),
        (yy_in.at[0], yy.at[0]), (q_in, query), (v_in, values), (persist_in, persist),
        *[(g_in.at[i], from_side.at[1, me.order(i)]) for i in range(EARLY)],
    )
    loads = [pltpu.make_async_copy(a, b, in_sem.at[i]) for i, (a, b) in enumerate(pairs)]
    for c in loads[1:3]:
        c.start()

    barrier = pltpu.get_barrier_semaphore()

    def greet(where):
        pl.semaphore_signal(barrier, inc=1, device_id=where, device_id_type=MESH)

    greet(me.at(line, side, 1 - core))
    greet(me.at(line, 1 - side, core))

    @pl.when(line > 0)
    def _():
        greet(me.at(line - 1, side, core))

    @pl.when(line < L - 1)
    def _():
        greet(me.at(line + 1, side, core))

    for peer in peers:
        greet(peer)
    ends = jnp.where(line > 0, 1, 0) + jnp.where(line < L - 1, 1, 0)
    pl.semaphore_wait(barrier, 2 + n_head - 1 + ends)
    for c in (loads[3], loads[4], loads[0], *loads[5:]):
        c.start()

    def rcopy(b, p):
        there = peers[p]["head"] * FB
        return remote(recall.at[there + b], got.at[head, b], x_send.at[p, b], x_recv.at[head, b], peers[p])

    for c in loads[1:3]:
        c.wait()

    mine = pl.ds(pl.multiple_of(core * R, R), R)
    theirs = pl.ds(pl.multiple_of((1 - core) * R, R), R)

    def core_copy(w, j):
        return remote(
            G.at[w, j, theirs, :], from_core.at[w, j], c_send.at[w, j], c_recv.at[w, j],
            me.at(line, side, 1 - core),
        )

    def side_copy(w, l):
        return remote(
            G.at[w, l * 2 + 1 - side, mine, :], from_side.at[w, l], s_send.at[w, l], s_recv.at[w, l],
            me.at(line, 1 - side, core),
        )

    def right_copy(w, l):
        return remote(
            G.at[w, l * 2 + side, mine, :], from_left.at[w, l], z_send.at[w, l], l_recv.at[w, l],
            me.at(line + 1, side, core),
        )

    def left_copy(w, l):
        return remote(
            G.at[w, l * 2 + side, mine, :], from_right.at[w, l], z_send.at[w, l], r_recv.at[w, l],
            me.at(line - 1, side, core),
        )

    def partial(w, j):
        G[w, j] = dot_tn(xx[w, j], yy[w]).astype(BF16)
        core_copy(w, j).start()

    there = 2 * L - EARLY
    far = L - 1
    at_end = (line == 0) | (line == L - 1)
    low = jnp.logical_not(at_end) & (line < L // 2)

    def across(n):
        both = 2 * (L - EARLY)
        n = jnp.where(low & (n == both - 1), both, jnp.where(low & (n == both), both - 1, n))
        w = jnp.where(n < both, 1 - n % 2, 0)
        return w, me.order(jnp.where(n < both, L - 1 - n // 2, EARLY - 1 - (n - both)))

    def along(n):
        t = n - (2 * far - 4)
        last_low = 2 * far - 4 + jnp.where(t % 2 == 0, 2 + t // 2, t // 2)
        last_high = 2 * far - 4 + (t % 2) * 2 + t // 2
        inner = jnp.where(t < 0, n, jnp.where(low, last_low, last_high))
        outer = jnp.where(n == 0, 2 * far - 2, jnp.where(n == 2 * far - 1, n, n - 1))
        q = jnp.where(at_end, outer, inner)
        own = n >= 2 * far
        return jnp.where(own, 1 - (n - 2 * far), 1 - q % 2), jnp.where(own, 0, L - 1 - q // 2)

    def line_partial(n):
        w, i = along(n)
        partial(w, me.order(i) * 2 + side)

    def line_finish(n):
        w, i = along(n)
        l = me.order(i)
        j = l * 2 + side
        core_copy(w, j).wait_recv()

        @pl.when((w == 0) | (i >= EARLY))
        def _():
            remote(
                from_side.at[w, l], from_side.at[w, l], s_send.at[w, l], s_recv.at[w, l],
                me.at(line, 1 - side, core),
            ).wait_recv()

        acc[...] = G[w, j, mine, :].astype(F32) + from_core[w, j].astype(F32) + from_side[w, l].astype(F32)

        @pl.when((l >= line) & (line > 0))
        def _():
            remote(
                from_left.at[w, l], from_left.at[w, l], z_send.at[w, l], l_recv.at[w, l],
                me.at(line - 1, side, core),
            ).wait_recv()
            acc[...] += from_left[w, l].astype(F32)

        @pl.when((l <= line) & (line < L - 1))
        def _():
            remote(
                from_right.at[w, l], from_right.at[w, l], z_send.at[w, l], r_recv.at[w, l],
                me.at(line + 1, side, core),
            ).wait_recv()
            acc[...] += from_right[w, l].astype(F32)

        @pl.when(l == line)
        def _():
            for tile in range(H // LANES):
                rows = pl.ds(tile * 2 + w, R, stride=2 * H // LANES)
                grad[rows, :] = acc[:, tile * LANES : (tile + 1) * LANES]

        @pl.when(l != line)
        def _():
            G[w, j, mine, :] = acc[...].astype(BF16)

        @pl.when(l > line)
        def _():
            right_copy(w, l).start()

        @pl.when(l < line)
        def _():
            left_copy(w, l).start()

    @pl.loop(0, there + 1)
    def _(n):
        @pl.when(n == 1)
        def _():
            loads[3].wait()
            loads[4].wait()

        @pl.when(n < there)
        def _():
            w, l = across(n)
            partial(w, l * 2 + 1 - side)

        @pl.when(n > 0)
        def _():
            w, l = across(n - 1)
            j = l * 2 + 1 - side
            core_copy(w, j).wait_recv()
            both = G[w, j, mine, :].astype(F32) + from_core[w, j].astype(F32)
            G[w, j, mine, :] = both.astype(BF16)
            side_copy(w, l).start()

        @pl.when((n == 1) & at_end)
        def _():
            line_partial(0)

        @pl.when(n == 2)
        def _():
            loads[0].wait()

            @pl.loop(0, FB)
            def _(b):
                for p in range(n_head - 1):
                    rcopy(b, p).start()

            for c in loads[8:]:
                c.wait()

        @pl.when((n == 2) & at_end)
        def _():
            line_finish(0)

    for c in loads[5:8]:
        c.wait()

    heads_here = FB * wide // HEAD_DIM
    per = wide // HEAD_DIM
    chunk = count // 2
    scale = HEAD_DIM ** (-0.5)
    persist_count = persist.shape[1]

    def attend(n):
        b = n // per
        cols = pl.ds(pl.multiple_of((n % per) * HEAD_DIM, HEAD_DIM), HEAD_DIM)
        flat = pl.ds(pl.multiple_of(n * HEAD_DIM, HEAD_DIM), HEAD_DIM)
        for part in range(2):
            seen = (part + 1) * chunk
            q = query[b, pl.ds(part * chunk, chunk), cols]
            row = lax.broadcasted_iota(jnp.int32, (chunk, seen), 0) + part * chunk
            visible = lax.broadcasted_iota(jnp.int32, (chunk, seen), 1) <= row
            rec = recalled[b, pl.ds(0, seen), cols]
            key = xx[0, base + b, pl.ds(0, seen), cols]
            val = values[b, pl.ds(0, seen), cols]
            s0 = dot_nt(q, persist[0, :, flat]) * scale
            s1 = jnp.where(visible, dot_nt(q, rec) * scale, -1e30)
            s2 = jnp.where(visible, dot_nt(q, key) * scale, -1e30)
            top = jnp.maximum(
                jnp.max(s0, axis=1, keepdims=True),
                jnp.maximum(jnp.max(s1, axis=1, keepdims=True), jnp.max(s2, axis=1, keepdims=True)),
            )
            e0, e1, e2 = jnp.exp(s0 - top), jnp.exp(s1 - top), jnp.exp(s2 - top)
            norm = 1.0 / (
                jnp.sum(e0, axis=1, keepdims=True)
                + jnp.sum(e1, axis=1, keepdims=True)
                + jnp.sum(e2, axis=1, keepdims=True)
            )
            out = dot((e0 * norm).astype(BF16), persist[1, :, flat])
            out = out + dot((e1 * norm).astype(BF16), rec)
            out = out + dot((e2 * norm).astype(BF16), val)
            attended[pl.ds(part * chunk, chunk), flat] = out.astype(BF16)

    def recall_all():
        @pl.loop(0, FB)
        def _(b):
            total = recall[base + b].astype(F32)
            for by in range(1, n_head):
                other = (head + by) % n_head
                remote(
                    got.at[other, b], got.at[other, b], x_send.at[0, b], x_recv.at[other, b], peers[0]
                ).wait_recv()
                total = total + got[other, b].astype(F32)
            recalled[b] = total.astype(BF16)

    each = -(-heads_here // 2)

    def sent():
        @pl.loop(0, FB)
        def _(b):
            for p in range(n_head - 1):
                rcopy(b, p).wait_send()

        @pl.loop(0, there)
        def _(n):
            w, l = across(n)
            core_copy(w, l * 2 + 1 - side).wait_send()
            side_copy(w, l).wait_send()

    @pl.loop(jnp.where(at_end, 1, 0), 2 * L)
    def _(n):
        line_partial(n)

        @pl.when(n == 2 * L - 1)
        def _():
            sent()

        @pl.when(n == far)
        def _():
            recall_all()

        @pl.loop(jnp.maximum((n - far) * each, 0), jnp.clip((n - far + 1) * each, 0, heads_here))
        def _(k):
            attend(k)

        line_finish(n)

    @pl.loop(0, L)
    def _(l):
        for w in range(2):
            core_copy(w, l * 2 + side).wait_send()

            @pl.when(l > line)
            def _():
                right_copy(w, l).wait_send()

            @pl.when(l < line)
            def _():
                left_copy(w, l).wait_send()


def backward(xx, yy, query, values, recall, early, persist, n_seq, n_head, R):
    _, chips, count, wide = xx.shape
    H, FB = yy.shape[2], query.shape[0]
    L = n_seq // 4
    anywhere = pl.BlockSpec(memory_space=pl.ANY)
    vmem = pl.BlockSpec(memory_space=pltpu.VMEM)
    S = jax.ShapeDtypeStruct
    dma = pltpu.SemaphoreType.DMA
    return pl.pallas_call(
        functools.partial(backward_kernel, n_seq, n_head),
        out_shape=(S((R * 2 * H // LANES, LANES), F32), S((count, FB * wide), BF16)),
        in_specs=[anywhere] * 7,
        out_specs=(vmem, vmem),
        scratch_shapes=[
            pltpu.VMEM(persist.shape, BF16),
            pltpu.VMEM((2, chips, count, wide), BF16),
            pltpu.VMEM((2, count, H), BF16),
            pltpu.VMEM((FB, count, wide), BF16),
            pltpu.VMEM((FB, count, wide), BF16),
            pltpu.VMEM((chips, count, wide), BF16),
            pltpu.VMEM((n_head, FB, count, wide), BF16),
            pltpu.VMEM((FB, count, wide), BF16),
            pltpu.VMEM((2, chips, wide, H), BF16),
            pltpu.VMEM((2, chips, R, H), BF16),
            pltpu.VMEM((2, L, R, H), BF16),
            pltpu.VMEM((2, L, R, H), BF16),
            pltpu.VMEM((2, L, R, H), BF16),
            pltpu.VMEM((R, H), F32),
            dma((2, chips)),
            dma((2, chips)),
            dma((2, L)),
            dma((2, L)),
            dma((2, L)),
            dma((2, L)),
            dma((2, L)),
            dma((max(n_head - 1, 1), FB)),
            dma((n_head, FB)),
            dma((8 + EARLY,)),
        ],
        compiler_params=pltpu.CompilerParams(
            collective_id=1, has_side_effects=True, vmem_limit_bytes=VMEM_LIMIT
        ),
    )(xx, yy, query, values, recall, early, persist)


def interleave(x):
    R, two, H = x.shape
    return x.reshape(R, two, H // LANES, LANES).transpose(0, 2, 1, 3).reshape(R * two * H // LANES, LANES)


def layered(x, R, H):
    return x.reshape(R, H // LANES, 2, LANES).transpose(0, 2, 1, 3).reshape(R, 2, H)


def update_kernel(decay, share, grad, memory, momentum, memory_out, momentum_out):
    new = decay[0] * momentum[...] - grad[...]
    momentum_out[...] = new
    memory_out[...] = (1.0 - share[0]) * memory[...] + new


def update(decay, share, grad, memory, momentum):
    rows = grad.shape[0]
    smem = pl.BlockSpec(memory_space=pltpu.SMEM)
    flat = pl.BlockSpec((rows // UPDATE_STEPS, LANES), lambda i: (i, 0))
    out = jax.ShapeDtypeStruct(grad.shape, F32)
    return pl.pallas_call(
        update_kernel,
        grid=(UPDATE_STEPS,),
        out_shape=(out, out),
        in_specs=[smem, smem, flat, flat, flat],
        out_specs=(flat, flat),
    )(decay, share, grad, memory, momentum)


def on_device(
    tokens, qkv_weight, persistent, rate_weight, forget_rate, momentum_decay, forget_share, memory, momentum
):
    n_seq, n_head = lax.axis_size("seq"), lax.axis_size("head")
    seg_len, width = tokens.shape[1], tokens.shape[2]
    lr_scale = 2.0 / (width * n_seq * seg_len) ** 0.5
    R, _, H = memory.shape
    memory_tiles = interleave(memory)
    qkv = jnp.transpose(qkv_weight, (1, 0, 2))
    xx, yy, query, values, recall, early = forward(
        tokens[0], qkv, memory_tiles, rate_weight[None], forget_rate, R, H, n_seq, n_head, lr_scale
    )
    grad, attended = backward(xx, yy, query, values, recall, early, persistent, n_seq, n_head, R)
    memory, momentum = update(momentum_decay, forget_share, grad, memory_tiles, interleave(momentum))
    memory, momentum = layered(memory, R, H), layered(momentum, R, H)
    return (attended[None], memory, momentum)


def solution(mesh):
    placed = (
        P(None, "seq", None),
        P(None, None, "head"),
        P(None, None, "head"),
        P(),
        P(None, "seq"),
        P(),
        P(),
        P("seq", None, "head"),
        P("seq", None, "head"),
    )
    return jax.shard_map(
        on_device,
        mesh=mesh,
        in_specs=placed,
        out_specs=(P(None, "seq", "head"), P("seq", None, "head"), P("seq", None, "head")),
        check_vma=False,
    )
```
